32 devices in a mesh: groups: 2 (over y), context: 16 (over z, x, core).
Axes of the slice: x: 2, y: 2, z: 4, core: 2. Of those that a mesh axis runs over, the one named last changes fastest.
Arguments:
- query_proj: bfloat16 [4096, 5120], P(('groups', 'context')), parts along dimension 0, may hold values from -100 to 100
- key_proj: bfloat16 [4096, 1024], P(('groups', 'context')), parts along dimension 0, may hold values from -100 to 100
- values: bfloat16 [4096, 1024], P(('groups', 'context')), parts along dimension 0, may hold values from -6 to 6
- grad_out: bfloat16 [4096, 5120], P(('groups', 'context')), parts along dimension 0, may hold values from -6 to 6
- query_gain: float32 [5120], replicated, may hold values from 0.1 to 1.9
- key_gain: float32 [1024], replicated, may hold values from 0.1 to 1.9
- segments: int32 [4096], P('groups'), parts along dimension 0, may hold values from 0 to 7, never falling along the last dimension, each value on 1 to 512 neighbouring positions
- layout: int32 [64], P('groups'), parts along dimension 0, may hold values from 0 to 31, as said below
Outputs:
- query_grad: bfloat16 [4096, 5120], P(('groups', 'context')), parts along dimension 0
- key_grad: bfloat16 [4096, 1024], P(('groups', 'context')), parts along dimension 0
- value_grad: bfloat16 [4096, 1024], P(('groups', 'context')), parts along dimension 0
- query_gain_grad: float32 [10240], P('groups'), parts along dimension 0
- key_gain_grad: float32 [2048], P('groups'), parts along dimension 0
The draws below stay inside these ranges and needn't reach their ends.
There are 2 independent parts, one for each index of `groups`. The reference program is written for one: setup_inputs(seed, part) draws one part's arguments, and reference() takes and returns one part's arrays. A program takes and returns all parts, laid end to end along the dimension named above; an argument that names none is the same for every part. Nothing has to cross between parts.
Inputs may be any that keep to these rules, and one draw needn't show every extreme that they name: layout is a permutation of the spans; slots are ordered device by device, 2 to a device, and each aligned run of 8 slots holds the spans of one sequence of 512 positions in some order. `segments`: document numbers never fall along the stream; a document has 1 to 512 positions, and one has exactly 512.
All inputs are finite; a program needn't handle non-finite values.
Results may differ from the reference program's by a relative error of at most 0.0086.
Values may be sent and summed in bfloat16 or wider, within the bound.
A program may use at most 128 MiB of HBM per device.

```python
import math
import jax
import jax.numpy as jnp
import numpy as np
from jax import lax

QUERY_HEADS = 40
KEY_VALUE_HEADS = 8
HEAD_SIZE = 128
SPAN = 64
CPD = 2
SEQ_DEVS = 4
QW = 5120
KW = 1024
TOK_DEV = 128
LENGTH = 512
STREAM_TOKENS = 2048
DOCS = 8
N_CONTEXT = 16


def draw_layout(key, part):
    window = SEQ_DEVS * CPD
    slot_count = STREAM_TOKENS // SPAN
    own_key = jax.random.fold_in(key, 3)
    scores = jax.random.randint(own_key, (slot_count // window, window), 0, 65536) * window + jnp.arange(window, dtype=jnp.int32)[None, :]
    local_order = jnp.argsort(scores, axis=1).astype(jnp.int32)
    starts = jnp.arange(slot_count // window, dtype=jnp.int32)[:, None] * window
    return (local_order + starts).reshape(slot_count).astype(jnp.int32)


def projection_sample(key, salt, width):
    own_key = jax.random.fold_in(key, salt)
    return jnp.clip(jax.random.normal(own_key, (STREAM_TOKENS, width)), -8.0, 8.0).astype(jnp.bfloat16)


def draw_query_proj(key, part):
    return projection_sample(key, 11, QUERY_HEADS * HEAD_SIZE)


def draw_key_proj(key, part):
    return projection_sample(key, 13, KEY_VALUE_HEADS * HEAD_SIZE)


def block_scale(rng, extent, split, low, top_value):
    loudness = 1.0
    for position, shards_of in split:
        steps = jax.random.uniform(jax.random.fold_in(jax.random.fold_in(rng, 6), position), (shards_of,), jnp.float32, low / len(split), top_value / len(split))
        loudness = loudness * jnp.repeat(jnp.exp(steps), extent[position] // shards_of).reshape((-1,) + (1,) * (len(extent) - 1 - position))
    return loudness


def split_up(amount, total, bound, slope):
    loads = [(1 << 20) // math.isqrt(standing ** slope) + 1 for standing in range(2, amount + 1)]
    rest, given = total - bound - (amount - 1), [1] * (amount - 1)
    while rest > 0:
        candidates = [i for i in range(amount - 1) if given[i] < bound]
        whole, budget = sum([loads[i] for i in candidates]), rest
        for i in candidates:
            more = min(bound - given[i], max(1, budget * loads[i] // whole), rest)
            given[i] = given[i] + more
            rest = rest - more
    return np.array([bound] + given)


def uneven_parts(rng, count, total, most, slope):
    if count == 2:
        one = jax.random.randint(rng, (), max(1, total - most), min(most, total - 1) + 1)
        return jnp.stack([one, total - one])
    lengths = jnp.asarray(split_up(count, total, most, slope), jnp.int32)
    twos = (count - 1) // 2
    giver, taker = lengths[1:1 + 2 * twos:2], lengths[2:2 + 2 * twos:2]
    room = jnp.minimum(giver - 1, most - taker)
    moved = jax.random.randint(jax.random.fold_in(rng, 1), (twos,), 0, 1 << 20) % (room + 1)
    lengths = lengths.at[1:1 + 2 * twos:2].set(giver - moved).at[2:2 + 2 * twos:2].set(taker + moved)
    return lengths[jax.random.permutation(jax.random.fold_in(rng, 2), count)]


def noise(key, shape, deviation, most, shards=(), kind=jnp.bfloat16):
    drawn = jax.random.normal(key, shape, jnp.float32) * deviation
    if len(shards) > 0:
        drawn = block_scale(key, shape, shards, -0.22, 0.18) * drawn
    return jnp.clip(drawn, min=-most, max=most).astype(kind)


def setup_inputs(seed: int = 0, part: int = 0) -> dict:
    keys = jax.random.split(jax.random.key(seed), 9)
    part_keys = jax.random.split(jax.random.fold_in(keys[8], part), 9)
    query_proj = draw_query_proj(jax.random.fold_in(jax.random.fold_in(keys[8], part), 71), part)
    key_proj = draw_key_proj(jax.random.fold_in(jax.random.fold_in(keys[8], part), 71), part)
    values = noise(part_keys[2], (STREAM_TOKENS, KW), 1.0, 6.0, ((0, 16),))
    grad_out = noise(part_keys[3], (STREAM_TOKENS, QW), 1.0, 6.0, ((0, 16),))
    query_gain = jnp.clip(1.0 + 0.18 * jax.random.normal(keys[4], (QW,), jnp.float32), 0.1, 1.9)
    key_gain = jnp.clip(1.0 + 0.18 * jax.random.normal(keys[5], (KW,), jnp.float32), 0.1, 1.9)
    segments = jnp.searchsorted(jnp.cumsum(uneven_parts(part_keys[6], DOCS, STREAM_TOKENS, LENGTH, 2)), jnp.arange(STREAM_TOKENS), side="right").astype(jnp.int32)
    layout = draw_layout(jax.random.fold_in(jax.random.fold_in(keys[8], part), 71), part)
    return {"query_proj": query_proj, "key_proj": key_proj, "values": values, "grad_out": grad_out, "query_gain": query_gain, "key_gain": key_gain, "segments": segments, "layout": layout}


NORM_EPS = 1e-06
ROPE_BASE = 500000.0

def rope_angles(positions, head_dim):
    half_dim = head_dim // 2
    inv_freq = jnp.power(ROPE_BASE, -2.0 * jnp.arange(half_dim, dtype=jnp.float32) / head_dim)
    angles = positions.astype(jnp.float32)[:, None] * inv_freq[None, :]
    return (jnp.cos(angles), jnp.sin(angles))

def rotate(inputs, cosine, sine, sign_flip):
    tok_rows = inputs.shape[0]
    half_dim = cosine.shape[1]
    halves = inputs.reshape(tok_rows, inputs.shape[1] // (2 * half_dim), 2, half_dim)
    lower_half = halves[:, :, 0]
    upper_half = halves[:, :, 1]
    cosine_b = cosine[:, None, :]
    sine_b = sine[:, None, :] * sign_flip
    rotated = jnp.stack([lower_half * cosine_b - upper_half * sine_b, upper_half * cosine_b + lower_half * sine_b], axis=2)
    return rotated.reshape(tok_rows, inputs.shape[1])

def norm_forward(inputs, gain_row):
    mean_sq = lax.optimization_barrier(jnp.mean(inputs * inputs, axis=1, keepdims=True))
    factor = lax.rsqrt(mean_sq + NORM_EPS)
    return (inputs * factor * gain_row[None, :], factor)

def norm_backward(inputs, factor, gain_row, upstream):
    weighted = upstream * gain_row[None, :]
    inner_sum = lax.optimization_barrier(jnp.mean(weighted * inputs, axis=1, keepdims=True))
    grad_in = factor * weighted - inputs * factor * factor * factor * inner_sum
    return (grad_in, lax.optimization_barrier(jnp.sum(upstream * inputs * factor, axis=0)))

def head_gradients(queries, key_rows, value_rows, grad_rows, allowed, query_head_group, head_dim):
    tok_rows = queries.shape[0]
    factor = head_dim ** (-0.5)
    query_heads = queries.reshape(tok_rows, query_head_group, head_dim).astype(jnp.float32)
    grad_heads = grad_rows.reshape(tok_rows, query_head_group, head_dim).astype(jnp.float32)
    key_float = key_rows.astype(jnp.float32)
    value_float = value_rows.astype(jnp.float32)
    scores = jnp.einsum('qgd,kd->gqk', query_heads, key_float) * factor
    scores = jnp.where(allowed[None], scores, -jnp.inf)
    row_max = lax.optimization_barrier(jnp.max(scores, axis=2, keepdims=True))
    expo = jnp.exp(scores - row_max)
    attn_probs = expo / lax.optimization_barrier(jnp.sum(expo, axis=2, keepdims=True))
    dprobs = jnp.einsum('qgd,kd->gqk', grad_heads, value_float)
    row_delta = lax.optimization_barrier(jnp.sum(attn_probs * dprobs, axis=2, keepdims=True))
    dscores = (attn_probs * (dprobs - row_delta)).astype(jnp.bfloat16).astype(jnp.float32)
    probs_low = attn_probs.astype(jnp.bfloat16).astype(jnp.float32)
    query_part = jnp.einsum('gqk,kd->qgd', dscores, key_float) * factor
    key_part = jnp.einsum('gqk,qgd->kd', dscores, query_heads) * factor
    value_part = jnp.einsum('gqk,qgd->kd', probs_low, grad_heads)
    return (query_part.reshape(tok_rows, query_head_group * head_dim), key_part, value_part)

def reference(query_proj, key_proj, values, grad_out, query_gain, key_gain, segments, layout):
    query_head_group = QUERY_HEADS // KEY_VALUE_HEADS
    group_width = query_head_group * HEAD_SIZE
    token_index = jnp.arange(STREAM_TOKENS, dtype=jnp.int32)
    positions = (jnp.take(layout, token_index // SPAN) * SPAN + token_index % SPAN).astype(jnp.int32)
    doc_ids = jnp.take(segments, positions)
    cosine, sine = rope_angles(positions % LENGTH, HEAD_SIZE)
    q_inputs = query_proj.astype(jnp.float32)
    k_inputs = key_proj.astype(jnp.float32)
    q_normed, q_factor = norm_forward(q_inputs, query_gain)
    k_normed, k_factor = norm_forward(k_inputs, key_gain)
    q_rope = rotate(q_normed, cosine, sine, 1.0).astype(jnp.bfloat16)
    k_rope = rotate(k_normed, cosine, sine, 1.0).astype(jnp.bfloat16)

    def block_step(carried, device):
        dk_acc, dv_acc = carried
        q_start = (device * TOK_DEV).astype(jnp.int32)
        k_start = (device // SEQ_DEVS * LENGTH).astype(jnp.int32)
        q_block = lax.dynamic_slice_in_dim(q_rope, q_start, TOK_DEV, 0)
        g_block = lax.dynamic_slice_in_dim(grad_out, q_start, TOK_DEV, 0)
        k_block = lax.dynamic_slice_in_dim(k_rope, k_start, LENGTH, 0)
        v_block = lax.dynamic_slice_in_dim(values, k_start, LENGTH, 0)
        pos_query = lax.dynamic_slice_in_dim(positions, q_start, TOK_DEV, 0)
        doc_query = lax.dynamic_slice_in_dim(doc_ids, q_start, TOK_DEV, 0)
        pos_key = lax.dynamic_slice_in_dim(positions, k_start, LENGTH, 0)
        doc_key = lax.dynamic_slice_in_dim(doc_ids, k_start, LENGTH, 0)
        same_seq = pos_key[None, :] // LENGTH == pos_query[:, None] // LENGTH
        allowed = same_seq & (doc_key[None, :] == doc_query[:, None]) & (pos_key[None, :] <= pos_query[:, None])
        query_parts, key_parts, value_parts = ([], [], [])
        for key_value_head in range(KEY_VALUE_HEADS):
            query_part, key_part, value_part = head_gradients(q_block[:, key_value_head * group_width:(key_value_head + 1) * group_width], k_block[:, key_value_head * HEAD_SIZE:(key_value_head + 1) * HEAD_SIZE], v_block[:, key_value_head * HEAD_SIZE:(key_value_head + 1) * HEAD_SIZE], g_block[:, key_value_head * group_width:(key_value_head + 1) * group_width], allowed, query_head_group, HEAD_SIZE)
            query_parts.append(query_part)
            key_parts.append(key_part)
            value_parts.append(value_part)
        key_block_grad = jnp.concatenate(key_parts, axis=1)
        value_block_grad = jnp.concatenate(value_parts, axis=1)
        dk_acc = lax.dynamic_update_slice_in_dim(dk_acc, lax.dynamic_slice_in_dim(dk_acc, k_start, LENGTH, 0) + key_block_grad, k_start, 0)
        dv_acc = lax.dynamic_update_slice_in_dim(dv_acc, lax.dynamic_slice_in_dim(dv_acc, k_start, LENGTH, 0) + value_block_grad, k_start, 0)
        return ((dk_acc, dv_acc), jnp.concatenate(query_parts, axis=1))
    key_zeros = jnp.zeros((STREAM_TOKENS, KEY_VALUE_HEADS * HEAD_SIZE), jnp.float32)
    (dk_rope, dv_sum), dq_blocks = lax.scan(block_step, (key_zeros, key_zeros), jnp.arange(N_CONTEXT, dtype=jnp.int32))
    dq_rope = dq_blocks.reshape(STREAM_TOKENS, QUERY_HEADS * HEAD_SIZE)
    dq_normed = rotate(dq_rope, cosine, sine, -1.0)
    dk_normed = rotate(dk_rope, cosine, sine, -1.0)
    query_grad, query_gain_grad = norm_backward(q_inputs, q_factor, query_gain, dq_normed)
    key_grad, key_gain_grad = norm_backward(k_inputs, k_factor, key_gain, dk_normed)
    return (query_grad.astype(jnp.bfloat16), key_grad.astype(jnp.bfloat16), dv_sum.astype(jnp.bfloat16), query_gain_grad, key_gain_grad)
```

```python
import functools
import math
import jax
import jax.numpy as jnp
import numpy as np
from jax import lax
from jax.experimental import pallas as pl
from jax.experimental.pallas import tpu as pltpu
from jax.sharding import PartitionSpec as P

HD = 128
KVH = 8
SPAN = 64
SEQ = 4
LENGTH = 512
EPS = 1e-06
AHEAD = 2
CHUNK = 2
BASE = 500000.0
F32 = jnp.float32
BF16 = jnp.bfloat16


def rope_tables():
    half = HD // 2
    freq = BASE ** (-2.0 * np.arange(half, dtype=np.float64) / HD)
    freq = np.concatenate([freq, freq])
    sign = np.concatenate([-np.ones(half), np.ones(half)])
    off = np.arange(SPAN)[:, None] * freq[None, :]
    start = np.arange(LENGTH // SPAN)[:, None] * SPAN * freq[None, :]
    return (
        np.stack([np.cos(off), np.sin(off) * sign]).astype(np.float32),
        np.stack([np.cos(start), np.sin(start) * sign]).astype(np.float32),
    )


def kernel(
    n_seq,
    layout_h, seg_h, q_h, k_h, v_h, g_h, qgain_h, kgain_h, t_off_h, t_start_h,
    qg_out, kg_out, vg_out, qgg_out, kgg_out,
    kv, bias, cs, qs, gs, u, r0, r2, rs13, rr13, rs2, rr2, gseq, gz, ds_a, p_a, ds_b, p_b, accq, rqb,
    s_x, r_x, s_c, r_c, s_f, r_f, s_13, r_13, s_2, r_2, s_g, r_g, s_z, r_z,
    layout, seg, q_in, k_in, g_in, qgain, kgain, t_off, t_start, l_sem, v_sem, ready, z_ready, z_known,
):
    rows = q_in.shape[0]
    qw = q_in.shape[1]
    kw = k_in.shape[1]
    group = qw // kw
    spans = rows // SPAN
    per_seq = LENGTH // SPAN
    gw = group * HD
    nq = qw // HD
    scale = HD ** (-0.5)
    me = lax.axis_index("context")
    rank = lax.rem(me, SEQ)
    base = me - rank
    my_seq = base // SEQ
    lead = lax.rem(rank, 2) == 1

    def flip(bit):
        if bit == 1:
            return rank + 1 - 2 * lax.rem(rank, 2)
        if bit == 2:
            return lax.rem(rank + 2, 4)
        return 3 - rank

    peer = {j: base + flip(j) for j in (1, 2, 3)}
    zpeer = [lax.rem(my_seq + i, n_seq) * SEQ + rank for i in range(1, n_seq)]

    def rcopy(src, dst, ss, rs, dev):
        return pltpu.make_async_remote_copy(
            src_ref=src, dst_ref=dst, send_sem=ss, recv_sem=rs,
            device_id={"context": dev}, device_id_type=pl.DeviceIdType.MESH,
        )

    def tell(sem, dev):
        pl.semaphore_signal(sem, inc=1, device_id={"context": dev}, device_id_type=pl.DeviceIdType.MESH)

    barrier = pltpu.get_barrier_semaphore()

    @pl.when(lead)
    def _():
        tell(barrier, peer[1])
        tell(barrier, peer[3])
        for z in zpeer:
            tell(barrier, z)

    @pl.when(jnp.logical_not(lead))
    def _():
        tell(barrier, peer[2])

    pairs = [
        (k_h, k_in), (layout_h, layout), (t_start_h, t_start), (t_off_h, t_off), (kgain_h, kgain),
        (seg_h, seg), (qgain_h, qgain), (q_h, q_in), (g_h, g_in),
    ]
    loads = [pltpu.make_async_copy(a, b, l_sem.at[i]) for i, (a, b) in enumerate(pairs)]
    v_loads = [
        pltpu.make_async_copy(v_h.at[:, pl.ds(h * HD, HD)], kv.at[h, 0, 1], v_sem.at[h]) for h in range(KVH)
    ]
    for c in loads[:5] + v_loads + loads[5:]:
        c.start()

    owners = [me, peer[1], peer[2], peer[3]]

    def factors(j):
        for i in range(spans):
            span = lax.rem(layout[owners[j] * spans + i], per_seq)
            c1, s1 = t_start[0, pl.ds(span, 1), :], t_start[1, pl.ds(span, 1), :]
            c2, s2 = t_off[0], t_off[1]
            cs[j, 0, i * SPAN : (i + 1) * SPAN, :] = c1 * c2 - s1 * s2
            cs[j, 1, i * SPAN : (i + 1) * SPAN, :] = s1 * c2 + c1 * s2

    def rot(x):
        return x * cs[0, 0] + pltpu.roll(x, HD // 2, 1) * cs[0, 1]

    def unrot(x, j=0):
        return x * cs[j, 0] - pltpu.roll(x, HD // 2, 1) * cs[j, 1]

    for c in loads[:5]:
        c.wait()
    factors(0)
    kf = k_in[...].astype(F32)
    rk = lax.rsqrt(jnp.sum(kf * kf, axis=1, keepdims=True) / kw + EPS)

    def x_copy(h, t):
        return rcopy(kv.at[h, 0, t], kv.at[h, 2, t], s_x.at[h, t], r_x.at[h, t], peer[2])

    def c_copy(h):
        return rcopy(kv.at[h, 0], kv.at[h, 1], s_c.at[h], r_c.at[h], peer[1])

    def f_copy(h):
        return rcopy(kv.at[h, 2], kv.at[h, 3], s_f.at[h], r_f.at[h], peer[1])

    def copy13(h):
        return rcopy(rs13.at[h], rr13.at[h], s_13.at[h], r_13.at[h], peer[1])

    def copy2(h):
        return rcopy(rs2.at[h], rr2.at[h], s_2.at[h], r_2.at[h], peer[2])

    def prepare_k(h):
        x = k_in[:, h * HD : (h + 1) * HD].astype(F32) * rk * kgain[h : h + 1, :]
        kv[h, 0, 0] = rot(x).astype(BF16)

    for h in range(AHEAD):
        prepare_k(h)
    for h in range(AHEAD):
        v_loads[h].wait()

    @pl.when(jnp.logical_not(lead))
    def _():
        pl.semaphore_wait(barrier, 3)
        tell(ready, peer[1])

    @pl.when(lead)
    def _():
        pl.semaphore_wait(ready, 1)

    for h in range(KVH):
        if h >= AHEAD:
            prepare_k(h)
            v_loads[h].wait()
        x_copy(h, 1).start()
        x_copy(h, 0).start()
        c_copy(h).start()
    for c in loads[5:]:
        c.wait()
    for j in (1, 2, 3):
        factors(j)

    lane = lax.broadcasted_iota(jnp.int32, (1, HD), 1)
    sub = lax.broadcasted_iota(jnp.int32, (rows, 1), 0)

    def docs_of(owner):
        row = jnp.zeros((1, HD), jnp.int32)
        for i in range(spans):
            sp = layout[owner * spans + i]
            src = seg[pl.ds(sp // 2, 1), :]
            swp = pltpu.roll(src, SPAN, 1)
            want = jnp.where(lax.rem(sp, 2) == i, src, swp)
            row = jnp.where(lane // SPAN == i, want, row)
        return row

    def pos_of(owner, idx):
        out = idx
        for i in range(spans):
            out = jnp.where(idx // SPAN == i, layout[owner * spans + i] * SPAN + idx - i * SPAN, out)
        return out

    doc_q = docs_of(me)
    pos_q = pos_of(me, lane)
    doc_rows = jnp.concatenate(
        [docs_of(o).astype(F32) for o in owners] + [jnp.zeros((4, HD), F32)], axis=0
    )
    doc_cols = jnp.transpose(doc_rows)
    doc_qf = doc_q.astype(F32)
    for j in range(SEQ):
        ok = (doc_cols[:, j : j + 1] == doc_qf) & (pos_of(owners[j], sub) <= pos_q)
        bias[j * rows : (j + 1) * rows, :] = jnp.where(ok, 0.0, -jnp.inf).astype(F32)

    ssq = jnp.zeros((rows, HD), F32)
    for i in range(nq):
        x = q_in[:, i * HD : (i + 1) * HD].astype(F32)
        ssq = ssq + x * x
    rq = lax.rsqrt(jnp.sum(ssq, axis=1, keepdims=True) / qw + EPS)
    rqb[...] = jnp.broadcast_to(rq, (rows, HD))
    accq[...] = jnp.zeros((rows, HD), F32)

    def prepare_q(h, carry):
        for g in range(group):
            at = pl.multiple_of(h * gw + g * HD, HD)
            x = q_in[:, pl.ds(at, HD)].astype(F32) * rqb[...] * qgain[pl.ds(h * group + g, 1), :]
            qs[h, g * rows : (g + 1) * rows, :] = rot(x).astype(BF16)
            gs[h, g * rows : (g + 1) * rows, :] = g_in[:, pl.ds(at, HD)]
        return carry

    lax.fori_loop(0, KVH, prepare_q, 0)

    nt = (((1,), (1,)), ((), ()))
    tn = (((0,), (0,)), ((), ()))
    chunks = [(a, min(a + CHUNK, group)) for a in range(0, group, CHUNK)]

    def forward(h):
        x_copy(h, 0).wait_recv()
        x_copy(h, 1).wait_recv()
        f_copy(h).start()

    def arrive(h):
        c_copy(h).wait_recv()
        f_copy(h).wait_recv()

    def relay(h):
        copy13(h).wait_recv()
        rs2[h] = (r2[h] + rr13[h, 1].astype(F32)).astype(BF16)
        r0[h] = r0[h] + rr13[h, 0].astype(F32)
        copy2(h).start()

    def scores(h, a, b):
        keys = kv[h, :, 0].reshape(SEQ * rows, HD)
        vals = kv[h, :, 1].reshape(SEQ * rows, HD)
        cols = slice(a * rows, b * rows)
        s = lax.dot_general(keys, qs[h, cols, :], nt, preferred_element_type=F32)
        dp = lax.dot_general(vals, gs[h, cols, :], nt, preferred_element_type=F32)
        return s, dp

    def weights(s, dp, a, b, ds_ref, p_ref):
        cols = slice(a * rows, b * rows)
        s = s * (scale * math.log2(math.e)) + jnp.concatenate([bias[...]] * (b - a), axis=1)
        e = jnp.exp2(s - jnp.max(s, axis=0, keepdims=True))
        p = e * (1.0 / jnp.sum(e, axis=0, keepdims=True))
        delta = jnp.sum(p * dp, axis=0, keepdims=True)
        ds_ref[:, cols] = (p * (dp - delta)).astype(BF16)
        p_ref[:, cols] = p.astype(BF16)

    def softmax(h, ds_ref, p_ref):
        for a, b in chunks:
            weights(*scores(h, a, b), a, b, ds_ref, p_ref)

    def key_products(h, ds_ref, p_ref):
        dk = jnp.dot(ds_ref[...], qs[h], preferred_element_type=F32) * scale
        r0[h, 0] = dk[:rows]
        rs13[h, 0, 0] = dk[rows : 2 * rows].astype(BF16)
        r2[h, 0] = dk[2 * rows : 3 * rows]
        rs13[h, 1, 0] = dk[3 * rows :].astype(BF16)
        kpart = jnp.zeros((rows, HD), F32)
        for j in range(SEQ):
            kpart = kpart + unrot(dk[j * rows : (j + 1) * rows], j) * unrot(kv[h, j, 0].astype(F32), j)
        gz[my_seq, pl.ds(nq + h, 1), :] = jnp.sum(kpart, axis=0, keepdims=True) / kgain[pl.ds(h, 1), :]

    def value_products(h, p_ref):
        dv = jnp.dot(p_ref[...], gs[h], preferred_element_type=F32)
        r0[h, 1] = dv[:rows]
        rs13[h, 0, 1] = dv[rows : 2 * rows].astype(BF16)
        r2[h, 1] = dv[2 * rows : 3 * rows]
        rs13[h, 1, 1] = dv[3 * rows :].astype(BF16)

    def query_products(h, ds_ref):
        keys = kv[h, :, 0].reshape(SEQ * rows, HD)
        return lax.dot_general(keys, ds_ref[...], tn, preferred_element_type=F32) * scale

    def query_side(h, dq_t):
        acc = accq[...]
        for g in range(group):
            at = pl.multiple_of(h * gw + g * HD, HD)
            dqn = unrot(jnp.transpose(dq_t[:, g * HD : (g + 1) * HD]))
            x = q_in[:, pl.ds(at, HD)].astype(F32)
            w = dqn * qgain[pl.ds(h * group + g, 1), :]
            u[:, pl.ds(at, HD)] = w
            acc = acc + w * x
            gz[my_seq, pl.ds(h * group + g, 1), :] = jnp.sum(dqn * x * rqb[...], axis=0, keepdims=True)
        accq[...] = acc

    slots = ((ds_a, p_a), (ds_b, p_b))

    def step(h, now, nxt):
        sc = scores(h + 1, *chunks[0])
        dq_t = query_products(h, now[0])
        weights(*sc, *chunks[0], *nxt)
        sc = scores(h + 1, *chunks[1])
        key_products(h, *now)
        query_side(h, dq_t)
        weights(*sc, *chunks[1], *nxt)
        sc = scores(h + 1, *chunks[2])
        value_products(h, now[1])
        weights(*sc, *chunks[2], *nxt)
        copy13(h).start()

    def meet(h):
        forward(h + 1)
        arrive(h)

    forward(0)
    arrive(0)
    softmax(0, *slots[0])
    forward(1)

    def two(i, carry):
        h = 2 * i
        meet(h + 1)

        @pl.when(i > 0)
        def _():
            relay(h - 1)

        step(h, slots[0], slots[1])
        meet(h + 2)
        relay(h)
        step(h + 1, slots[1], slots[0])
        return carry

    half = (KVH - 2) // 2
    lax.fori_loop(0, half, two, 0)

    @pl.when(lead)
    def _():
        pl.semaphore_wait(barrier, n_seq - 1)
        for z in zpeer:
            tell(z_ready, z)

    arrive(KVH - 1)
    relay(KVH - 3)
    step(KVH - 2, slots[0], slots[1])

    @pl.when(lead)
    def _():
        pl.semaphore_wait(z_ready, n_seq - 1)
        tell(z_known, peer[1])

    key_products(KVH - 1, *slots[1])
    value_products(KVH - 1, slots[1][1])
    copy13(KVH - 1).start()
    relay(KVH - 2)
    query_side(KVH - 1, query_products(KVH - 1, slots[1][0]))

    @pl.when(jnp.logical_not(lead))
    def _():
        pl.semaphore_wait(z_known, 1)

    def gc_copy():
        return rcopy(gseq.at[0], gseq.at[1], s_g.at[0], r_g.at[0], peer[1])

    def gx_copy():
        return rcopy(gseq.at[2], gseq.at[3], s_g.at[1], r_g.at[1], peer[2])

    def z_copy(i):
        return rcopy(gz.at[my_seq], gz.at[my_seq], s_z.at[i], r_z.at[i], zpeer[i])

    def z_recv(i):
        src = lax.rem(my_seq + n_seq - 1 - i, n_seq)
        return rcopy(gz.at[my_seq], gz.at[src], s_z.at[i], r_z.at[i], src * SEQ + rank)

    for i in range(n_seq - 1):
        z_copy(i).start()
    relay(KVH - 1)
    rq = rqb[...]
    inner = jnp.sum(accq[...], axis=1, keepdims=True) / qw * rq * rq * rq
    for i in range(nq):
        sl = slice(i * HD, (i + 1) * HD)
        qg_out[:, sl] = (rq * u[:, sl] - q_in[:, sl].astype(F32) * inner).astype(BF16)

    kacc = jnp.zeros((rows, HD), F32)

    def finish(h, kacc):
        sl = slice(h * HD, (h + 1) * HD)
        copy2(h).wait_recv()
        vg_out[:, sl] = (r0[h, 1] + rr2[h, 1].astype(F32)).astype(BF16)
        dkn = unrot(r0[h, 0] + rr2[h, 0].astype(F32))
        x = k_in[:, sl].astype(F32)
        w = dkn * kgain[h : h + 1, :]
        r2[h, 0] = w
        return kacc + w * x

    early = KVH - 2
    for h in range(early):
        kacc = finish(h, kacc)

    for i in range(n_seq - 1):
        z_recv(i).wait_recv()
    total = gz[0]
    for s_i in range(1, n_seq):
        total = total + gz[s_i]
    gseq[0] = total
    gc_copy().start()
    kacc = finish(early, kacc)
    gc_copy().wait_recv()
    gseq[2] = gseq[0] + gseq[1]
    gx_copy().start()
    kacc = finish(early + 1, kacc)

    kinner = jnp.sum(kacc, axis=1, keepdims=True) / kw * rk * rk * rk
    for h in range(KVH):
        sl = slice(h * HD, (h + 1) * HD)
        kg_out[:, sl] = (rk * r2[h, 0] - k_in[:, sl].astype(F32) * kinner).astype(BF16)

    gx_copy().wait_recv()
    total = gseq[2] + gseq[3]
    qgg_out[...] = total[:nq]
    kgg_out[...] = total[nq:]

    for h in range(KVH):
        x_copy(h, 0).wait_send()
        x_copy(h, 1).wait_send()
        c_copy(h).wait_send()
        f_copy(h).wait_send()
        copy13(h).wait_send()
        copy2(h).wait_send()
    gc_copy().wait_send()
    gx_copy().wait_send()
    for i in range(n_seq - 1):
        z_copy(i).wait_send()


def flush(*refs):
    sems = refs[10]
    copies = [pltpu.make_async_copy(refs[i], refs[5 + i], sems.at[i]) for i in range(5)]
    for c in copies:
        c.start()
    for c in copies:
        c.wait()


def body(n_ctx, query_proj, key_proj, values, grad_out, query_gain, key_gain, segments, layout):
    rows, qw = query_proj.shape
    kw = key_proj.shape[1]
    group = qw // kw
    n_seq = n_ctx // SEQ
    nq, nk = qw // HD, kw // HD
    t_off, t_start = rope_tables()
    vmem = pl.BlockSpec(memory_space=pltpu.VMEM)
    sem = pltpu.SemaphoreType.DMA
    outs = pl.pallas_call(
        functools.partial(kernel, n_seq),
        out_shape=(
            pltpu.VMEM((rows, qw), BF16),
            pltpu.VMEM((rows, kw), BF16),
            pltpu.VMEM((rows, kw), BF16),
            pltpu.VMEM((nq, HD), F32),
            pltpu.VMEM((nk, HD), F32),
        ),
        in_specs=[pl.BlockSpec(memory_space=pltpu.HBM)] * 10,
        out_specs=(vmem,) * 5,
        scratch_shapes=[
            pltpu.VMEM((nk, SEQ, 2, rows, HD), BF16),
            pltpu.VMEM((SEQ * rows, rows), F32),
            pltpu.VMEM((SEQ, 2, rows, HD), F32),
            pltpu.VMEM((nk, group * rows, HD), BF16),
            pltpu.VMEM((nk, group * rows, HD), BF16),
            pltpu.VMEM((rows, qw), F32),
            pltpu.VMEM((nk, 2, rows, HD), F32),
            pltpu.VMEM((nk, 2, rows, HD), F32),
            pltpu.VMEM((nk, 2, 2, rows, HD), BF16),
            pltpu.VMEM((nk, 2, 2, rows, HD), BF16),
            pltpu.VMEM((nk, 2, rows, HD), BF16),
            pltpu.VMEM((nk, 2, rows, HD), BF16),
            pltpu.VMEM((SEQ, nq + nk, HD), F32),
            pltpu.VMEM((n_seq, nq + nk, HD), F32),
        ]
        + [pltpu.VMEM((SEQ * rows, group * rows), BF16)] * 4
        + [pltpu.VMEM((rows, HD), F32)] * 2
        + [sem((nk, 2))] * 2
        + [sem((nk,))] * 8
        + [sem((2,))] * 2
        + [sem((max(n_seq - 1, 1),))] * 2
        + [
            pltpu.SMEM(layout.shape, jnp.int32),
            pltpu.VMEM((segments.shape[0] // HD, HD), jnp.int32),
            pltpu.VMEM((rows, qw), BF16),
            pltpu.VMEM((rows, kw), BF16),
            pltpu.VMEM((rows, qw), BF16),
            pltpu.VMEM((nq, HD), F32),
            pltpu.VMEM((nk, HD), F32),
            pltpu.VMEM(t_off.shape, F32),
            pltpu.VMEM(t_start.shape, F32),
            sem((9,)),
            sem((nk,)),
        ]
        + [pltpu.SemaphoreType.REGULAR] * 3,
        compiler_params=pltpu.CompilerParams(
            collective_id=0, has_side_effects=True, vmem_limit_bytes=65100000
        ),
    )(
        layout, segments.reshape(-1, HD), query_proj, key_proj, values, grad_out,
        query_gain.reshape(nq, HD), key_gain.reshape(nk, HD), jnp.asarray(t_off), jnp.asarray(t_start),
    )
    anyspace = pl.BlockSpec(memory_space=pl.ANY)
    outs = pl.pallas_call(
        flush,
        out_shape=tuple(jax.ShapeDtypeStruct(o.shape, o.dtype) for o in outs),
        in_specs=[anyspace] * 5,
        out_specs=(anyspace,) * 5,
        scratch_shapes=[sem((5,))],
        compiler_params=pltpu.CompilerParams(vmem_limit_bytes=8 * 1024 * 1024),
    )(*outs)
    return outs[0], outs[1], outs[2], outs[3].reshape(qw), outs[4].reshape(kw)


def solution(mesh):
    tok = P(("groups", "context"), None)
    return jax.shard_map(
        functools.partial(body, mesh.shape["context"]),
        mesh=mesh,
        in_specs=(tok, tok, tok, tok, P(), P(), P("groups"), P("groups")),
        out_specs=(tok, tok, tok, P("groups"), P("groups")),
        check_vma=False,
    )
```

```python
import functools
import math
import jax
import jax.numpy as jnp
import numpy as np
from jax import lax
from jax.experimental import pallas as pl
from jax.experimental.pallas import tpu as pltpu
from jax.sharding import PartitionSpec as P

HD = 128
KVH = 8
SPAN = 64
SEQ = 4
LENGTH = 512
EPS = 1e-06
AHEAD = 2
CHUNK = 3
BASE = 500000.0
F32 = jnp.float32
BF16 = jnp.bfloat16


def rope_tables():
    half = HD // 2
    freq = BASE ** (-2.0 * np.arange(half, dtype=np.float64) / HD)
    freq = np.concatenate([freq, freq])
    sign = np.concatenate([-np.ones(half), np.ones(half)])
    off = np.arange(SPAN)[:, None] * freq[None, :]
    start = np.arange(LENGTH // SPAN)[:, None] * SPAN * freq[None, :]
    return (
        np.stack([np.cos(off), np.sin(off) * sign]).astype(np.float32),
        np.stack([np.cos(start), np.sin(start) * sign]).astype(np.float32),
    )


def kernel(
    n_seq,
    layout_h, seg_h, q_h, k_h, v_h, g_h, qgain_h, kgain_h, t_off_h, t_start_h,
    qg_out, kg_out, vg_out, qgg_out, kgg_out,
    kv, bias, cs, qs, gs, u, r0, r2, rs13, rr13, rs2, rr2, gseq, gz, ds_a, p_a, ds_b, p_b, accq, rqb, glast,
    s_x, s_c, s_f, s_13, s_2, s_l, r_l, r_x, r_cf, r_13, r_2, s_g, r_g, s_z, r_z,
    layout, seg, q_in, k_in, g_in, qgain, kgain, t_off, t_start, l_sem, v_sem, ready, z_ready, z_known,
):
    rows = q_in.shape[0]
    qw = q_in.shape[1]
    kw = k_in.shape[1]
    group = qw // kw
    spans = rows // SPAN
    per_seq = LENGTH // SPAN
    gw = group * HD
    nq = qw // HD
    scale = HD ** (-0.5)
    me = lax.axis_index("context")
    rank = lax.rem(me, SEQ)
    base = me - rank
    my_seq = base // SEQ
    lead = lax.rem(rank, 2) == 1

    def flip(bit):
        if bit == 1:
            return rank + 1 - 2 * lax.rem(rank, 2)
        if bit == 2:
            return lax.rem(rank + 2, 4)
        return 3 - rank

    peer = {j: base + flip(j) for j in (1, 2, 3)}
    zpeer = [lax.rem(my_seq + i, n_seq) * SEQ + rank for i in range(1, n_seq)]

    def rcopy(src, dst, ss, rs, dev):
        return pltpu.make_async_remote_copy(
            src_ref=src, dst_ref=dst, send_sem=ss, recv_sem=rs,
            device_id={"context": dev}, device_id_type=pl.DeviceIdType.MESH,
        )

    def tell(sem, dev):
        pl.semaphore_signal(sem, inc=1, device_id={"context": dev}, device_id_type=pl.DeviceIdType.MESH)

    barrier = pltpu.get_barrier_semaphore()

    @pl.when(lead)
    def _():
        tell(barrier, peer[1])
        tell(barrier, peer[3])
        for z in zpeer:
            tell(barrier, z)

    @pl.when(jnp.logical_not(lead))
    def _():
        tell(barrier, peer[2])

    pairs = [
        (k_h, k_in), (layout_h, layout), (t_start_h, t_start), (t_off_h, t_off), (kgain_h, kgain),
        (seg_h, seg), (qgain_h, qgain), (q_h, q_in), (g_h, g_in),
    ]
    loads = [pltpu.make_async_copy(a, b, l_sem.at[i]) for i, (a, b) in enumerate(pairs)]
    v_loads = [
        pltpu.make_async_copy(v_h.at[:, pl.ds(h * HD, HD)], kv.at[h, 0, 1], v_sem) for h in range(KVH)
    ]
    for c in loads[:5] + v_loads + loads[5:]:
        c.start()

    owners = [me, peer[2], peer[1], peer[3]]

    def factors(j):
        for i in range(spans):
            span = lax.rem(layout[owners[j] * spans + i], per_seq)
            c1, s1 = t_start[0, pl.ds(span, 1), :], t_start[1, pl.ds(span, 1), :]
            c2, s2 = t_off[0], t_off[1]
            cs[j, 0, i * SPAN : (i + 1) * SPAN, :] = c1 * c2 - s1 * s2
            cs[j, 1, i * SPAN : (i + 1) * SPAN, :] = s1 * c2 + c1 * s2

    def rot(x):
        return x * cs[0, 0] + pltpu.roll(x, HD // 2, 1) * cs[0, 1]

    def unrot(x, j=0):
        return x * cs[j, 0] - pltpu.roll(x, HD // 2, 1) * cs[j, 1]

    for c in loads[:5]:
        c.wait()
    factors(0)
    kf = k_in[...].astype(F32)
    rk = lax.rsqrt(jnp.sum(kf * kf, axis=1, keepdims=True) / kw + EPS)

    def x_copy(h, t):
        return rcopy(kv.at[h, 0, t], kv.at[h, 1, t], s_x, r_x.at[h], peer[2])

    def c_copy(h):
        return rcopy(kv.at[h, 0], kv.at[h, 2], s_c, r_cf.at[h], peer[1])

    def f_copy(h):
        return rcopy(kv.at[h, 1], kv.at[h, 3], s_f, r_cf.at[h], peer[1])

    def copy13(h):
        return rcopy(rs13.at[h], rr13.at[h], s_13, r_13.at[h], peer[1])

    def copy2(h):
        return rcopy(rs2.at[h], rr2.at[h], s_2, r_2.at[h], peer[2])

    def prepare_k(h):
        x = k_in[:, h * HD : (h + 1) * HD].astype(F32) * rk * kgain[h : h + 1, :]
        kv[h, 0, 0] = rot(x).astype(BF16)

    for h in range(AHEAD):
        prepare_k(h)
    pltpu.make_async_copy(kv.at[:, 0, 1], kv.at[:, 0, 1], v_sem).wait()

    @pl.when(jnp.logical_not(lead))
    def _():
        pl.semaphore_wait(barrier, 3)
        tell(ready, peer[1])

    @pl.when(lead)
    def _():
        pl.semaphore_wait(ready, 1)

    for h in range(KVH):
        if h >= AHEAD:
            prepare_k(h)
        x_copy(h, 1).start()
        x_copy(h, 0).start()
        c_copy(h).start()
    for c in loads[5:]:
        c.wait()
    for j in (1, 2, 3):
        factors(j)

    lane = lax.broadcasted_iota(jnp.int32, (1, HD), 1)
    sub = lax.broadcasted_iota(jnp.int32, (rows, 1), 0)

    def docs_of(owner):
        row = jnp.zeros((1, HD), jnp.int32)
        for i in range(spans):
            sp = layout[owner * spans + i]
            src = seg[pl.ds(sp // 2, 1), :]
            swp = pltpu.roll(src, SPAN, 1)
            want = jnp.where(lax.rem(sp, 2) == i, src, swp)
            row = jnp.where(lane // SPAN == i, want, row)
        return row

    def pos_of(owner, idx):
        out = idx
        for i in range(spans):
            out = jnp.where(idx // SPAN == i, layout[owner * spans + i] * SPAN + idx - i * SPAN, out)
        return out

    doc_q = docs_of(me)
    pos_q = pos_of(me, lane)
    doc_rows = jnp.concatenate(
        [docs_of(o).astype(F32) for o in owners] + [jnp.zeros((4, HD), F32)], axis=0
    )
    doc_cols = jnp.transpose(doc_rows)
    doc_qf = doc_q.astype(F32)
    for j in range(SEQ):
        ok = (doc_cols[:, j : j + 1] == doc_qf) & (pos_of(owners[j], sub) <= pos_q)
        bias[j * rows : (j + 1) * rows, :] = jnp.where(ok, 0.0, -jnp.inf).astype(F32)

    ssq = jnp.zeros((rows, HD), F32)
    for i in range(nq):
        x = q_in[:, i * HD : (i + 1) * HD].astype(F32)
        ssq = ssq + x * x
    rq = lax.rsqrt(jnp.sum(ssq, axis=1, keepdims=True) / qw + EPS)
    rqb[...] = jnp.broadcast_to(rq, (rows, HD))
    accq[...] = jnp.zeros((rows, HD), F32)

    def prepare_q(h, carry):
        for g in range(group):
            at = pl.multiple_of(h * gw + g * HD, HD)
            x = q_in[:, pl.ds(at, HD)].astype(F32) * rqb[...] * qgain[pl.ds(h * group + g, 1), :]
            qs[h, g * rows : (g + 1) * rows, :] = rot(x).astype(BF16)
            gs[h, g * rows : (g + 1) * rows, :] = g_in[:, pl.ds(at, HD)]
        return carry

    lax.fori_loop(0, KVH, prepare_q, 0)

    nt = (((1,), (1,)), ((), ()))
    tn = (((0,), (0,)), ((), ()))
    chunks = [(a, min(a + CHUNK, group)) for a in range(0, group, CHUNK)]

    def forward(h):
        rcopy(kv.at[h, 0], kv.at[h, 1], s_x, r_x.at[h], peer[2]).wait_recv()
        f_copy(h).start()

    def arrive(h):
        rcopy(kv.at[h, pl.ds(0, 2)], kv.at[h, pl.ds(2, 2)], s_c, r_cf.at[h], peer[1]).wait_recv()

    def relay(h):
        copy13(h).wait_recv()
        rs2[h] = (r2[h] + rr13[h, 1].astype(F32)).astype(BF16)
        r0[h] = r0[h] + rr13[h, 0].astype(F32)
        copy2(h).start()

    def scores(h, a, b):
        keys = kv[h, :, 0].reshape(SEQ * rows, HD)
        vals = kv[h, :, 1].reshape(SEQ * rows, HD)
        cols = slice(a * rows, b * rows)
        s = lax.dot_general(keys, qs[h, cols, :], nt, preferred_element_type=F32)
        dp = lax.dot_general(vals, gs[h, cols, :], nt, preferred_element_type=F32)
        return s, dp

    def weights(s, dp, a, b, ds_ref, p_ref):
        cols = slice(a * rows, b * rows)
        s = s * (scale * math.log2(math.e)) + jnp.concatenate([bias[...]] * (b - a), axis=1)
        e = jnp.exp2(s - jnp.max(s, axis=0, keepdims=True))
        inv = 1.0 / jnp.sum(e, axis=0, keepdims=True)
        delta = jnp.sum(e * dp, axis=0, keepdims=True) * inv
        p = e * inv
        ds_ref[:, cols] = (p * (dp - delta)).astype(BF16)
        p_ref[:, cols] = p.astype(BF16)

    def softmax(h, ds_ref, p_ref):
        for a, b in chunks:
            weights(*scores(h, a, b), a, b, ds_ref, p_ref)

    def key_products(h, ds_ref, p_ref):
        dk = jnp.dot(ds_ref[...], qs[h], preferred_element_type=F32) * scale
        r0[h, 0] = dk[:rows]
        r2[h, 0] = dk[rows : 2 * rows]
        rs13[h, 0, 0] = dk[2 * rows : 3 * rows].astype(BF16)
        rs13[h, 1, 0] = dk[3 * rows :].astype(BF16)
        return dk

    def key_gains(h, dk):
        kpart = jnp.zeros((rows, HD), F32)
        for j in range(SEQ):
            kpart = kpart + unrot(dk[j * rows : (j + 1) * rows], j) * unrot(kv[h, j, 0].astype(F32), j)
        gz[my_seq, h, group : group + 1, :] = jnp.sum(kpart, axis=0, keepdims=True) / kgain[pl.ds(h, 1), :]

    def value_products(h, p_ref):
        dv = jnp.dot(p_ref[...], gs[h], preferred_element_type=F32)
        r0[h, 1] = dv[:rows]
        r2[h, 1] = dv[rows : 2 * rows]
        rs13[h, 0, 1] = dv[2 * rows : 3 * rows].astype(BF16)
        rs13[h, 1, 1] = dv[3 * rows :].astype(BF16)

    def query_products(h, ds_ref):
        keys = kv[h, :, 0].reshape(SEQ * rows, HD)
        return lax.dot_general(keys, ds_ref[...], tn, preferred_element_type=F32) * scale

    def query_side(h, dq_t):
        acc = accq[...]
        for g in range(group):
            at = pl.multiple_of(h * gw + g * HD, HD)
            dqn = unrot(jnp.transpose(dq_t[:, g * HD : (g + 1) * HD]))
            x = q_in[:, pl.ds(at, HD)].astype(F32)
            w = dqn * qgain[pl.ds(h * group + g, 1), :]
            u[:, pl.ds(at, HD)] = w
            acc = acc + w * x
            gz[my_seq, h, g : g + 1, :] = jnp.sum(dqn * x * rqb[...], axis=0, keepdims=True)
        accq[...] = acc

    parts = (pl.ds(0, KVH - 1), pl.ds(KVH - 1, 1))

    def z_copy(i, t):
        mine = gz.at[my_seq, parts[t]]
        return rcopy(mine, mine, s_z.at[t], r_z.at[t], zpeer[i])

    def z_all(t):
        others = gz.at[pl.ds(0, n_seq - 1), parts[t]]
        return rcopy(others, others, s_z.at[t], r_z.at[t], zpeer[0])

    slots = ((ds_a, p_a), (ds_b, p_b))

    def step(h, now, nxt):
        sc = scores(h + 1, *chunks[0])
        dq_t = query_products(h, now[0])
        weights(*sc, *chunks[0], *nxt)
        sc = scores(h + 1, *chunks[1])
        dk = key_products(h, *now)
        query_side(h, dq_t)
        weights(*sc, *chunks[1], *nxt)
        value_products(h, now[1])
        key_gains(h, dk)
        copy13(h).start()

    def meet(h):
        forward(h + 1)
        arrive(h)

    forward(0)
    arrive(0)
    softmax(0, *slots[0])
    forward(1)

    def two(i, carry):
        h = 2 * i
        meet(h + 1)

        @pl.when(i > 0)
        def _():
            relay(h - 2)

        step(h, slots[0], slots[1])
        meet(h + 2)

        @pl.when(i > 0)
        def _():
            relay(h - 1)

        step(h + 1, slots[1], slots[0])
        return carry

    @pl.when(lead)
    def _():
        pl.semaphore_wait(barrier, n_seq - 1)
        for z in zpeer:
            tell(z_ready, z)

    half = (KVH - 2) // 2
    lax.fori_loop(0, half, two, 0)

    @pl.when(lead)
    def _():
        pl.semaphore_wait(z_ready, n_seq - 1)
        tell(z_known, peer[1])

    arrive(KVH - 1)
    relay(KVH - 4)
    step(KVH - 2, slots[0], slots[1])

    @pl.when(jnp.logical_not(lead))
    def _():
        pl.semaphore_wait(z_known, 1)

    for i in range(n_seq - 1):
        z_copy(i, 0).start()
    relay(KVH - 3)
    dk_last = key_products(KVH - 1, *slots[1])
    value_products(KVH - 1, slots[1][1])
    key_gains(KVH - 1, dk_last)
    copy13(KVH - 1).start()
    relay(KVH - 2)
    query_side(KVH - 1, query_products(KVH - 1, slots[1][0]))

    def gc_copy():
        return rcopy(gseq.at[0], gseq.at[1], s_g.at[0], r_g.at[0], peer[1])

    def gx_copy():
        return rcopy(gseq.at[2], gseq.at[3], s_g.at[1], r_g.at[1], peer[2])

    def gl_copy(j):
        return rcopy(glast.at[0], glast.at[j], s_l, r_l, peer[j])

    def over_z(t):
        z_all(t).wait_recv()
        total = gz[0, parts[t]]
        for s_i in range(1, n_seq):
            total = total + gz[s_i, parts[t]]
        return total

    for i in range(n_seq - 1):
        z_copy(i, 1).start()
    relay(KVH - 1)
    rq = rqb[...]
    inner = jnp.sum(accq[...], axis=1, keepdims=True) / qw * rq * rq * rq
    for i in range(nq):
        sl = slice(i * HD, (i + 1) * HD)
        qg_out[:, sl] = (rq * u[:, sl] - q_in[:, sl].astype(F32) * inner).astype(BF16)

    kacc = jnp.zeros((rows, HD), F32)

    def finish(h, kacc):
        sl = slice(h * HD, (h + 1) * HD)
        copy2(h).wait_recv()
        vg_out[:, sl] = (r0[h, 1] + rr2[h, 1].astype(F32)).astype(BF16)
        dkn = unrot(r0[h, 0] + rr2[h, 0].astype(F32))
        x = k_in[:, sl].astype(F32)
        w = dkn * kgain[h : h + 1, :]
        r2[h, 0] = w
        return kacc + w * x

    early = KVH - 2
    for h in range(early):
        kacc = finish(h, kacc)
    rcopy(kv.at[:, 0], kv.at[:, 1], s_x, r_x.at[0], peer[2]).wait_send()
    rcopy(kv.at[:, 0], kv.at[:, 2], s_c, r_cf.at[0], peer[1]).wait_send()
    rcopy(kv.at[:, 1], kv.at[:, 3], s_f, r_cf.at[0], peer[1]).wait_send()
    rcopy(rs13, rr13, s_13, r_13.at[0], peer[1]).wait_send()

    gseq[0] = over_z(0)
    gc_copy().start()
    gc_copy().wait_recv()
    gseq[2] = gseq[0] + gseq[1]
    gx_copy().start()
    kacc = finish(early, kacc)
    glast[0] = over_z(1)
    for j in (2, 3, 1):
        gl_copy(j).start()
    kacc = finish(early + 1, kacc)

    kinner = jnp.sum(kacc, axis=1, keepdims=True) / kw * rk * rk * rk
    for h in range(KVH):
        sl = slice(h * HD, (h + 1) * HD)
        kg_out[:, sl] = (rk * r2[h, 0] - k_in[:, sl].astype(F32) * kinner).astype(BF16)

    gx_copy().wait_recv()
    gl_all = rcopy(glast.at[pl.ds(1, 3)], glast.at[pl.ds(1, 3)], s_l, r_l, peer[1])
    gl_all.wait_recv()
    for h in range(KVH):
        if h == KVH - 1:
            rows_h = glast[0, 0] + glast[1, 0] + (glast[2, 0] + glast[3, 0])
        else:
            rows_h = gseq[2, h] + gseq[3, h]
        qgg_out[h * group : (h + 1) * group, :] = rows_h[:group]
        kgg_out[h : h + 1, :] = rows_h[group : group + 1]

    rcopy(rs2, rr2, s_2, r_2.at[0], peer[2]).wait_send()
    gc_copy().wait_send()
    gx_copy().wait_send()
    gl_all.wait_send()
    z_all(0).wait_send()
    z_all(1).wait_send()


def flush(*refs):
    sems = refs[10]
    copies = [pltpu.make_async_copy(refs[i], refs[5 + i], sems.at[i]) for i in range(5)]
    for c in copies:
        c.start()
    for c in copies:
        c.wait()


def body(n_ctx, query_proj, key_proj, values, grad_out, query_gain, key_gain, segments, layout):
    rows, qw = query_proj.shape
    kw = key_proj.shape[1]
    group = qw // kw
    n_seq = n_ctx // SEQ
    nq, nk = qw // HD, kw // HD
    t_off, t_start = rope_tables()
    vmem = pl.BlockSpec(memory_space=pltpu.VMEM)
    sem = pltpu.SemaphoreType.DMA
    outs = pl.pallas_call(
        functools.partial(kernel, n_seq),
        out_shape=(
            pltpu.VMEM((rows, qw), BF16),
            pltpu.VMEM((rows, kw), BF16),
            pltpu.VMEM((rows, kw), BF16),
            pltpu.VMEM((nq, HD), F32),
            pltpu.VMEM((nk, HD), F32),
        ),
        in_specs=[pl.BlockSpec(memory_space=pltpu.HBM)] * 10,
        out_specs=(vmem,) * 5,
        scratch_shapes=[
            pltpu.VMEM((nk, SEQ, 2, rows, HD), BF16),
            pltpu.VMEM((SEQ * rows, rows), F32),
            pltpu.VMEM((SEQ, 2, rows, HD), F32),
            pltpu.VMEM((nk, group * rows, HD), BF16),
            pltpu.VMEM((nk, group * rows, HD), BF16),
            pltpu.VMEM((rows, qw), F32),
            pltpu.VMEM((nk, 2, rows, HD), F32),
            pltpu.VMEM((nk, 2, rows, HD), F32),
            pltpu.VMEM((nk, 2, 2, rows, HD), BF16),
            pltpu.VMEM((nk, 2, 2, rows, HD), BF16),
            pltpu.VMEM((nk, 2, rows, HD), BF16),
            pltpu.VMEM((nk, 2, rows, HD), BF16),
            pltpu.VMEM((SEQ, nk - 1, group + 1, HD), F32),
            pltpu.VMEM((n_seq, nk, group + 1, HD), F32),
        ]
        + [pltpu.VMEM((SEQ * rows, group * rows), BF16)] * 4
        + [pltpu.VMEM((rows, HD), F32)] * 2
        + [pltpu.VMEM((SEQ, 1, group + 1, HD), F32)]
        + [sem] * 7
        + [sem((nk,))] * 4
        + [sem((2,))] * 4
        + [
            pltpu.SMEM(layout.shape, jnp.int32),
            pltpu.VMEM((segments.shape[0] // HD, HD), jnp.int32),
            pltpu.VMEM((rows, qw), BF16),
            pltpu.VMEM((rows, kw), BF16),
            pltpu.VMEM((rows, qw), BF16),
            pltpu.VMEM((nq, HD), F32),
            pltpu.VMEM((nk, HD), F32),
            pltpu.VMEM(t_off.shape, F32),
            pltpu.VMEM(t_start.shape, F32),
            sem((9,)),
            sem,
        ]
        + [pltpu.SemaphoreType.REGULAR] * 3,
        compiler_params=pltpu.CompilerParams(
            collective_id=0, has_side_effects=True, vmem_limit_bytes=65100000
        ),
    )(
        layout, segments.reshape(-1, HD), query_proj, key_proj, values, grad_out,
        query_gain.reshape(nq, HD), key_gain.reshape(nk, HD), jnp.asarray(t_off), jnp.asarray(t_start),
    )
    anyspace = pl.BlockSpec(memory_space=pl.ANY)
    outs = pl.pallas_call(
        flush,
        out_shape=tuple(jax.ShapeDtypeStruct(o.shape, o.dtype) for o in outs),
        in_specs=[anyspace] * 5,
        out_specs=(anyspace,) * 5,
        scratch_shapes=[sem((5,))],
        compiler_params=pltpu.CompilerParams(vmem_limit_bytes=8 * 1024 * 1024),
    )(*outs)
    return outs[0], outs[1], outs[2], outs[3].reshape(qw), outs[4].reshape(kw)


def solution(mesh):
    tok = P(("groups", "context"), None)
    return jax.shard_map(
        functools.partial(body, mesh.shape["context"]),
        mesh=mesh,
        in_specs=(tok, tok, tok, tok, P(), P(), P("groups"), P("groups")),
        out_specs=(tok, tok, tok, P("groups"), P("groups")),
        check_vma=False,
    )
```

```python
import functools
import math
import jax
import jax.numpy as jnp
import numpy as np
from jax import lax
from jax.experimental import pallas as pl
from jax.experimental.pallas import tpu as pltpu
from jax.sharding import PartitionSpec as P

HD = 128
KVH = 8
SPAN = 64
SEQ = 4
LENGTH = 512
EPS = 1e-06
AHEAD = 2
CHUNK = 3
BASE = 500000.0
F32 = jnp.float32
BF16 = jnp.bfloat16


def rope_tables():
    half = HD // 2
    freq = BASE ** (-2.0 * np.arange(half, dtype=np.float64) / HD)
    freq = np.concatenate([freq, freq])
    sign = np.concatenate([-np.ones(half), np.ones(half)])
    off = np.arange(SPAN)[:, None] * freq[None, :]
    start = np.arange(LENGTH // SPAN)[:, None] * SPAN * freq[None, :]
    return (
        np.stack([np.cos(off), np.sin(off) * sign]).astype(np.float32),
        np.stack([np.cos(start), np.sin(start) * sign]).astype(np.float32),
    )


def kernel(
    n_seq,
    layout_h, seg_h, q_h, k_h, v_h, g_h, qgain_h, kgain_h, t_off_h, t_start_h,
    qg_out, kg_out, vg_out, qgg_out, kgg_out,
    kv, bias, cs, qs, gs, u, r0, r2, rs13, rr13, rs2, rr2, gseq, gz, ds_a, p_a, ds_b, p_b, accq, rqb, glast, glz,
    s_x, s_c, s_f, s_13, s_2, s_l, r_l, r_x, r_cf, r_13, r_2, s_g, r_g, s_z, r_z,
    layout, seg, q_in, k_in, g_in, qgain, kgain, t_off, t_start, l_sem, v_sem, ready, z_ready, z_known,
):
    rows = q_in.shape[0]
    qw = q_in.shape[1]
    kw = k_in.shape[1]
    group = qw // kw
    spans = rows // SPAN
    per_seq = LENGTH // SPAN
    gw = group * HD
    nq = qw // HD
    scale = HD ** (-0.5)
    me = lax.axis_index("context")
    rank = lax.rem(me, SEQ)
    base = me - rank
    my_seq = base // SEQ
    lead = lax.rem(rank, 2) == 0
    near = lax.rem(rank, 2) == 1

    def flip(bit):
        if bit == 1:
            return rank + 1 - 2 * lax.rem(rank, 2)
        if bit == 2:
            return lax.rem(rank + 2, 4)
        return 3 - rank

    peer = {j: base + flip(j) for j in (1, 2, 3)}
    zpeer = [lax.rem(my_seq + i, n_seq) * SEQ + rank for i in range(1, n_seq)]

    def rcopy(src, dst, ss, rs, dev):
        return pltpu.make_async_remote_copy(
            src_ref=src, dst_ref=dst, send_sem=ss, recv_sem=rs,
            device_id={"context": dev}, device_id_type=pl.DeviceIdType.MESH,
        )

    def tell(sem, dev):
        pl.semaphore_signal(sem, inc=1, device_id={"context": dev}, device_id_type=pl.DeviceIdType.MESH)

    barrier = pltpu.get_barrier_semaphore()

    @pl.when(lead)
    def _():
        tell(barrier, peer[1])
        tell(barrier, peer[3])
        for z in zpeer:
            tell(barrier, z)

    @pl.when(jnp.logical_not(lead))
    def _():
        tell(barrier, peer[2])

    pairs = [
        (k_h, k_in), (layout_h, layout), (t_start_h, t_start), (t_off_h, t_off), (kgain_h, kgain),
        (seg_h, seg), (qgain_h, qgain), (q_h, q_in), (g_h, g_in),
    ]
    loads = [pltpu.make_async_copy(a, b, l_sem.at[i]) for i, (a, b) in enumerate(pairs)]
    v_loads = [
        pltpu.make_async_copy(v_h.at[:, pl.ds(h * HD, HD)], kv.at[h, 0, 1], v_sem) for h in range(KVH)
    ]
    for c in loads[:5] + v_loads + loads[5:]:
        c.start()

    owners = [me, peer[2], peer[1], peer[3]]

    def factors(j):
        for i in range(spans):
            span = lax.rem(layout[owners[j] * spans + i], per_seq)
            c1, s1 = t_start[0, pl.ds(span, 1), :], t_start[1, pl.ds(span, 1), :]
            c2, s2 = t_off[0], t_off[1]
            cs[j, 0, i * SPAN : (i + 1) * SPAN, :] = c1 * c2 - s1 * s2
            cs[j, 1, i * SPAN : (i + 1) * SPAN, :] = s1 * c2 + c1 * s2

    def rot(x):
        return x * cs[0, 0] + pltpu.roll(x, HD // 2, 1) * cs[0, 1]

    def unrot(x, j=0):
        return x * cs[j, 0] - pltpu.roll(x, HD // 2, 1) * cs[j, 1]

    for c in loads[:5]:
        c.wait()
    factors(0)
    kf = k_in[...].astype(F32)
    rk = lax.rsqrt(jnp.sum(kf * kf, axis=1, keepdims=True) / kw + EPS)

    def x_copy(h, t):
        return rcopy(kv.at[h, 0, t], kv.at[h, 1, t], s_x, r_x.at[h], peer[2])

    def c_copy(h):
        return rcopy(kv.at[h, 0], kv.at[h, 2], s_c, r_cf.at[h], peer[1])

    def f_copy(h):
        return rcopy(kv.at[h, 1], kv.at[h, 3], s_f, r_cf.at[h], peer[1])

    def copy13(h):
        return rcopy(rs13.at[h], rr13.at[h], s_13, r_13.at[h], peer[1])

    def copy2(h):
        return rcopy(rs2.at[h], rr2.at[h], s_2, r_2.at[h], peer[2])

    def prepare_k(h):
        x = k_in[:, h * HD : (h + 1) * HD].astype(F32) * rk * kgain[h : h + 1, :]
        kv[h, 0, 0] = rot(x).astype(BF16)

    for h in range(AHEAD):
        prepare_k(h)
    pltpu.make_async_copy(kv.at[:, 0, 1], kv.at[:, 0, 1], v_sem).wait()

    @pl.when(jnp.logical_not(lead))
    def _():
        pl.semaphore_wait(barrier, 3)
        tell(ready, peer[1])

    @pl.when(lead)
    def _():
        pl.semaphore_wait(ready, 1)

    for h in range(KVH):
        if h >= AHEAD:
            prepare_k(h)
        x_copy(h, 1).start()
        x_copy(h, 0).start()
        c_copy(h).start()
    for c in loads[5:]:
        c.wait()
    for j in (1, 2, 3):
        factors(j)

    lane = lax.broadcasted_iota(jnp.int32, (1, HD), 1)
    sub = lax.broadcasted_iota(jnp.int32, (rows, 1), 0)

    def docs_of(owner):
        row = jnp.zeros((1, HD), jnp.int32)
        for i in range(spans):
            sp = layout[owner * spans + i]
            src = seg[pl.ds(sp // 2, 1), :]
            swp = pltpu.roll(src, SPAN, 1)
            want = jnp.where(lax.rem(sp, 2) == i, src, swp)
            row = jnp.where(lane // SPAN == i, want, row)
        return row

    def pos_of(owner, idx):
        out = idx
        for i in range(spans):
            out = jnp.where(idx // SPAN == i, layout[owner * spans + i] * SPAN + idx - i * SPAN, out)
        return out

    doc_q = docs_of(me)
    pos_q = pos_of(me, lane)
    doc_rows = jnp.concatenate(
        [docs_of(o).astype(F32) for o in owners] + [jnp.zeros((4, HD), F32)], axis=0
    )
    doc_cols = jnp.transpose(doc_rows)
    doc_qf = doc_q.astype(F32)
    for j in range(SEQ):
        ok = (doc_cols[:, j : j + 1] == doc_qf) & (pos_of(owners[j], sub) <= pos_q)
        bias[j * rows : (j + 1) * rows, :] = jnp.where(ok, 0.0, -jnp.inf).astype(F32)

    ssq = jnp.zeros((rows, HD), F32)
    for i in range(nq):
        x = q_in[:, i * HD : (i + 1) * HD].astype(F32)
        ssq = ssq + x * x
    rq = lax.rsqrt(jnp.sum(ssq, axis=1, keepdims=True) / qw + EPS)
    rqb[...] = jnp.broadcast_to(rq, (rows, HD))
    accq[...] = jnp.zeros((rows, HD), F32)

    def prepare_q(h, carry):
        for g in range(group):
            at = pl.multiple_of(h * gw + g * HD, HD)
            x = q_in[:, pl.ds(at, HD)].astype(F32) * rqb[...] * qgain[pl.ds(h * group + g, 1), :]
            qs[h, g * rows : (g + 1) * rows, :] = rot(x).astype(BF16)
            gs[h, g * rows : (g + 1) * rows, :] = g_in[:, pl.ds(at, HD)]
        return carry

    lax.fori_loop(0, KVH, prepare_q, 0)

    nt = (((1,), (1,)), ((), ()))
    tn = (((0,), (0,)), ((), ()))
    chunks = [(a, min(a + CHUNK, group)) for a in range(0, group, CHUNK)]

    def forward(h):
        rcopy(kv.at[h, 0], kv.at[h, 1], s_x, r_x.at[h], peer[2]).wait_recv()
        f_copy(h).start()

    def arrive(h):
        rcopy(kv.at[h, pl.ds(0, 2)], kv.at[h, pl.ds(2, 2)], s_c, r_cf.at[h], peer[1]).wait_recv()

    def relay(h):
        copy13(h).wait_recv()
        rs2[h] = (r2[h] + rr13[h, 1].astype(F32)).astype(BF16)
        r0[h] = r0[h] + rr13[h, 0].astype(F32)
        copy2(h).start()

    def scores(h, a, b):
        keys = kv[h, :, 0].reshape(SEQ * rows, HD)
        vals = kv[h, :, 1].reshape(SEQ * rows, HD)
        cols = slice(a * rows, b * rows)
        s = lax.dot_general(keys, qs[h, cols, :], nt, preferred_element_type=F32)
        dp = lax.dot_general(vals, gs[h, cols, :], nt, preferred_element_type=F32)
        return s, dp

    def weights(s, dp, a, b, ds_ref, p_ref):
        cols = slice(a * rows, b * rows)
        s = s * (scale * math.log2(math.e)) + jnp.concatenate([bias[...]] * (b - a), axis=1)
        e = jnp.exp2(s - jnp.max(s, axis=0, keepdims=True))
        inv = 1.0 / jnp.sum(e, axis=0, keepdims=True)
        delta = jnp.sum(e * dp, axis=0, keepdims=True) * inv
        p = e * inv
        ds_ref[:, cols] = (p * (dp - delta)).astype(BF16)
        p_ref[:, cols] = p.astype(BF16)

    def softmax(h, ds_ref, p_ref):
        for a, b in chunks:
            weights(*scores(h, a, b), a, b, ds_ref, p_ref)

    def key_products(h, ds_ref, p_ref):
        dk = jnp.dot(ds_ref[...], qs[h], preferred_element_type=F32) * scale
        r0[h, 0] = dk[:rows]
        r2[h, 0] = dk[rows : 2 * rows]
        rs13[h, 0, 0] = dk[2 * rows : 3 * rows].astype(BF16)
        rs13[h, 1, 0] = dk[3 * rows :].astype(BF16)
        return dk

    def key_gains(h, dk):
        kpart = jnp.zeros((rows, HD), F32)
        for j in range(SEQ):
            kpart = kpart + unrot(dk[j * rows : (j + 1) * rows], j) * unrot(kv[h, j, 0].astype(F32), j)
        gz[my_seq, h, group : group + 1, :] = jnp.sum(kpart, axis=0, keepdims=True) / kgain[pl.ds(h, 1), :]

    def value_products(h, p_ref):
        dv = jnp.dot(p_ref[...], gs[h], preferred_element_type=F32)
        r0[h, 1] = dv[:rows]
        r2[h, 1] = dv[rows : 2 * rows]
        rs13[h, 0, 1] = dv[2 * rows : 3 * rows].astype(BF16)
        rs13[h, 1, 1] = dv[3 * rows :].astype(BF16)

    def query_products(h, ds_ref):
        keys = kv[h, :, 0].reshape(SEQ * rows, HD)
        return lax.dot_general(keys, ds_ref[...], tn, preferred_element_type=F32) * scale

    def query_side(h, dq_t):
        acc = accq[...]
        for g in range(group):
            at = pl.multiple_of(h * gw + g * HD, HD)
            dqn = unrot(jnp.transpose(dq_t[:, g * HD : (g + 1) * HD]))
            x = q_in[:, pl.ds(at, HD)].astype(F32)
            w = dqn * qgain[pl.ds(h * group + g, 1), :]
            u[:, pl.ds(at, HD)] = w
            acc = acc + w * x
            gz[my_seq, h, g : g + 1, :] = jnp.sum(dqn * x * rqb[...], axis=0, keepdims=True)
        accq[...] = acc

    early_rows = pl.ds(0, KVH - 2)
    slot = my_seq * 2 + lax.rem(rank, 2)
    side = [peer[1]]
    for i in range(1, n_seq):
        side += [zpeer[i - 1], zpeer[i - 1] - rank + flip(1)]

    def z_copy(i):
        mine = gz.at[my_seq, early_rows]
        return rcopy(mine, mine, s_z.at[0], r_z.at[0], zpeer[i])

    def z_all():
        others = gz.at[pl.ds(0, n_seq - 1), early_rows]
        return rcopy(others, others, s_z.at[0], r_z.at[0], zpeer[0])

    def last_copy(dev):
        return rcopy(gz.at[my_seq, pl.ds(KVH - 2, 2)], glz.at[slot], s_z.at[1], r_z.at[1], dev)

    def last_all():
        others = glz.at[pl.ds(0, 2 * n_seq - 1)]
        return rcopy(others, others, s_z.at[1], r_z.at[1], peer[1])

    slots = ((ds_a, p_a), (ds_b, p_b))

    def step(h, now, nxt):
        sc = scores(h + 1, *chunks[0])
        dq_t = query_products(h, now[0])
        weights(*sc, *chunks[0], *nxt)
        sc = scores(h + 1, *chunks[1])
        dk = key_products(h, *now)
        query_side(h, dq_t)
        weights(*sc, *chunks[1], *nxt)
        value_products(h, now[1])
        key_gains(h, dk)
        copy13(h).start()

    def meet(h):
        forward(h + 1)
        arrive(h)

    forward(0)
    arrive(0)
    softmax(0, *slots[0])
    forward(1)

    def two(i, carry):
        h = 2 * i

        @pl.when(jnp.logical_and(lead, i == half - 1))
        def _():
            pl.semaphore_wait(z_ready, n_seq - 1)
            tell(z_known, peer[1])

        meet(h + 1)

        @pl.when(i > 0)
        def _():
            relay(h - 2)

        step(h, slots[0], slots[1])
        meet(h + 2)

        @pl.when(i > 0)
        def _():
            relay(h - 1)

        step(h + 1, slots[1], slots[0])
        return carry

    @pl.when(lead)
    def _():
        pl.semaphore_wait(barrier, n_seq - 1)
        for z in zpeer:
            tell(z_ready, z)

    half = (KVH - 2) // 2
    lax.fori_loop(0, half, two, 0)

    @pl.when(jnp.logical_not(lead))
    def _():
        pl.semaphore_wait(z_known, 1)

    for i in range(n_seq - 1):
        z_copy(i).start()
    arrive(KVH - 1)
    relay(KVH - 4)
    step(KVH - 2, slots[0], slots[1])

    relay(KVH - 3)
    dk_last = key_products(KVH - 1, *slots[1])
    query_side(KVH - 1, query_products(KVH - 1, slots[1][0]))
    key_gains(KVH - 1, dk_last)
    glz[slot] = gz[my_seq, KVH - 2 :]
    for dev in side:
        last_copy(dev).start()
    relay(KVH - 2)
    value_products(KVH - 1, slots[1][1])
    copy13(KVH - 1).start()

    def gc_copy():
        return rcopy(gseq.at[0], gseq.at[1], s_g.at[0], r_g.at[0], peer[1])

    def gx_copy():
        return rcopy(gseq.at[2], gseq.at[3], s_g.at[1], r_g.at[1], peer[2])

    def gl_copy(j):
        return rcopy(glast.at[0], glast.at[1], s_l, r_l, peer[j])

    relay(KVH - 1)
    rq = rqb[...]
    inner = jnp.sum(accq[...], axis=1, keepdims=True) / qw * rq * rq * rq
    for i in range(nq):
        sl = slice(i * HD, (i + 1) * HD)
        qg_out[:, sl] = (rq * u[:, sl] - q_in[:, sl].astype(F32) * inner).astype(BF16)

    kacc = jnp.zeros((rows, HD), F32)

    def finish(h, kacc):
        sl = slice(h * HD, (h + 1) * HD)
        copy2(h).wait_recv()
        vg_out[:, sl] = (r0[h, 1] + rr2[h, 1].astype(F32)).astype(BF16)
        dkn = unrot(r0[h, 0] + rr2[h, 0].astype(F32))
        x = k_in[:, sl].astype(F32)
        w = dkn * kgain[h : h + 1, :]
        r2[h, 0] = w
        return kacc + w * x

    rcopy(kv.at[:, 0], kv.at[:, 1], s_x, r_x.at[0], peer[2]).wait_send()
    rcopy(kv.at[:, 0], kv.at[:, 2], s_c, r_cf.at[0], peer[1]).wait_send()
    rcopy(kv.at[:, 1], kv.at[:, 3], s_f, r_cf.at[0], peer[1]).wait_send()
    rcopy(rs13, rr13, s_13, r_13.at[0], peer[1]).wait_send()

    for h in range(3):
        kacc = finish(h, kacc)
    z_all().wait_recv()
    total = gz[0, early_rows]
    for s_i in range(1, n_seq):
        total = total + gz[s_i, early_rows]
    gseq[0] = total
    gc_copy().start()
    kacc = finish(3, kacc)
    kacc = finish(4, kacc)
    gc_copy().wait_recv()
    gseq[2] = gseq[0] + gseq[1]
    gx_copy().start()
    kacc = finish(KVH - 3, kacc)
    last_all().wait_recv()
    last = glz[0]
    for s_i in range(1, 2 * n_seq):
        last = last + glz[s_i]
    glast[0] = last

    @pl.when(near)
    def _():
        gl_copy(2).start()
        gl_copy(3).start()

    kacc = finish(KVH - 2, kacc)
    kacc = finish(KVH - 1, kacc)

    kinner = jnp.sum(kacc, axis=1, keepdims=True) / kw * rk * rk * rk
    for h in range(KVH):
        sl = slice(h * HD, (h + 1) * HD)
        kg_out[:, sl] = (rk * r2[h, 0] - k_in[:, sl].astype(F32) * kinner).astype(BF16)

    rcopy(rs2, rr2, s_2, r_2.at[0], peer[2]).wait_send()
    gc_copy().wait_send()
    z_all().wait_send()
    last_all().wait_send()

    def gains(h, rows_h):
        qgg_out[h * group : (h + 1) * group, :] = rows_h[:group]
        kgg_out[h : h + 1, :] = rows_h[group : group + 1]

    gx_copy().wait_recv()
    for h in range(KVH - 2):
        gains(h, gseq[2, h] + gseq[3, h])
    gx_copy().wait_send()
    gl_copy(2).wait_recv()
    for h in range(2):
        gains(KVH - 2 + h, glast[0, h] + glast[1, h])

    @pl.when(near)
    def _():
        rcopy(glast, glast, s_l, r_l, peer[2]).wait_send()


def flush(*refs):
    sems = refs[10]
    copies = [pltpu.make_async_copy(refs[i], refs[5 + i], sems.at[i]) for i in range(5)]
    for c in copies:
        c.start()
    for c in copies:
        c.wait()


def body(n_ctx, query_proj, key_proj, values, grad_out, query_gain, key_gain, segments, layout):
    rows, qw = query_proj.shape
    kw = key_proj.shape[1]
    group = qw // kw
    n_seq = n_ctx // SEQ
    nq, nk = qw // HD, kw // HD
    t_off, t_start = rope_tables()
    vmem = pl.BlockSpec(memory_space=pltpu.VMEM)
    sem = pltpu.SemaphoreType.DMA
    outs = pl.pallas_call(
        functools.partial(kernel, n_seq),
        out_shape=(
            pltpu.VMEM((rows, qw), BF16),
            pltpu.VMEM((rows, kw), BF16),
            pltpu.VMEM((rows, kw), BF16),
            pltpu.VMEM((nq, HD), F32),
            pltpu.VMEM((nk, HD), F32),
        ),
        in_specs=[pl.BlockSpec(memory_space=pltpu.HBM)] * 10,
        out_specs=(vmem,) * 5,
        scratch_shapes=[
            pltpu.VMEM((nk, SEQ, 2, rows, HD), BF16),
            pltpu.VMEM((SEQ * rows, rows), F32),
            pltpu.VMEM((SEQ, 2, rows, HD), F32),
            pltpu.VMEM((nk, group * rows, HD), BF16),
            pltpu.VMEM((nk, group * rows, HD), BF16),
            pltpu.VMEM((rows, qw), F32),
            pltpu.VMEM((nk, 2, rows, HD), F32),
            pltpu.VMEM((nk, 2, rows, HD), F32),
            pltpu.VMEM((nk, 2, 2, rows, HD), BF16),
            pltpu.VMEM((nk, 2, 2, rows, HD), BF16),
            pltpu.VMEM((nk, 2, rows, HD), BF16),
            pltpu.VMEM((nk, 2, rows, HD), BF16),
            pltpu.VMEM((SEQ, nk - 2, group + 1, HD), F32),
            pltpu.VMEM((n_seq, nk, group + 1, HD), F32),
        ]
        + [pltpu.VMEM((SEQ * rows, group * rows), BF16)] * 4
        + [pltpu.VMEM((rows, HD), F32)] * 2
        + [pltpu.VMEM((2, 2, group + 1, HD), F32), pltpu.VMEM((2 * n_seq, 2, group + 1, HD), F32)]
        + [sem] * 7
        + [sem((nk,))] * 4
        + [sem((2,))] * 4
        + [
            pltpu.SMEM(layout.shape, jnp.int32),
            pltpu.VMEM((segments.shape[0] // HD, HD), jnp.int32),
            pltpu.VMEM((rows, qw), BF16),
            pltpu.VMEM((rows, kw), BF16),
            pltpu.VMEM((rows, qw), BF16),
            pltpu.VMEM((nq, HD), F32),
            pltpu.VMEM((nk, HD), F32),
            pltpu.VMEM(t_off.shape, F32),
            pltpu.VMEM(t_start.shape, F32),
            sem((9,)),
            sem,
        ]
        + [pltpu.SemaphoreType.REGULAR] * 3,
        compiler_params=pltpu.CompilerParams(
            collective_id=0, has_side_effects=True, vmem_limit_bytes=65100000
        ),
    )(
        layout, segments.reshape(-1, HD), query_proj, key_proj, values, grad_out,
        query_gain.reshape(nq, HD), key_gain.reshape(nk, HD), jnp.asarray(t_off), jnp.asarray(t_start),
    )
    anyspace = pl.BlockSpec(memory_space=pl.ANY)
    outs = pl.pallas_call(
        flush,
        out_shape=tuple(jax.ShapeDtypeStruct(o.shape, o.dtype) for o in outs),
        in_specs=[anyspace] * 5,
        out_specs=(anyspace,) * 5,
        scratch_shapes=[sem((5,))],
        compiler_params=pltpu.CompilerParams(vmem_limit_bytes=8 * 1024 * 1024),
    )(*outs)
    return outs[0], outs[1], outs[2], outs[3].reshape(qw), outs[4].reshape(kw)


def solution(mesh):
    tok = P(("groups", "context"), None)
    return jax.shard_map(
        functools.partial(body, mesh.shape["context"]),
        mesh=mesh,
        in_specs=(tok, tok, tok, tok, P(), P(), P("groups"), P("groups")),
        out_specs=(tok, tok, tok, P("groups"), P("groups")),
        check_vma=False,
    )
```

```python
import functools
import math
import jax
import jax.numpy as jnp
import numpy as np
from jax import lax
from jax.experimental import pallas as pl
from jax.experimental.pallas import tpu as pltpu
from jax.sharding import PartitionSpec as P

HD = 128
KVH = 8
SPAN = 64
SEQ = 4
LENGTH = 512
EPS = 1e-06
AHEAD = 1
CHUNK = 3
BASE = 500000.0
F32 = jnp.float32
BF16 = jnp.bfloat16


def rope_tables():
    half = HD // 2
    freq = BASE ** (-2.0 * np.arange(half, dtype=np.float64) / HD)
    freq = np.concatenate([freq, freq])
    sign = np.concatenate([-np.ones(half), np.ones(half)])
    off = np.arange(SPAN)[:, None] * freq[None, :]
    start = np.arange(LENGTH // SPAN)[:, None] * SPAN * freq[None, :]
    return (
        np.stack([np.cos(off), np.sin(off) * sign]).astype(np.float32),
        np.stack([np.cos(start), np.sin(start) * sign]).astype(np.float32),
    )


def kernel(
    n_seq,
    layout_h, seg_h, q_h, k_h, v_h, g_h, qgain_h, kgain_h, t_off_h, t_start_h,
    qg_out, kg_out, vg_out, qgg_out, kgg_out,
    kv, bias, cs, qs, gs, u, r0, r2, rs13, rr13, rs2, rr2, gseq, gz, ds_a, p_a, ds_b, p_b, accq, rqb, glast, glz,
    s_x, s_c, s_f, s_13, s_2, s_l, r_l, r_x, r_cf, r_13, r_2, s_g, r_g, s_z, r_z,
    layout, seg, q_in, k_in, g_in, qgain, kgain, t_off, t_start, l_sem, v_sem, ready, z_ready, z_known,
):
    rows = q_in.shape[0]
    qw = q_in.shape[1]
    kw = k_in.shape[1]
    group = qw // kw
    spans = rows // SPAN
    per_seq = LENGTH // SPAN
    gw = group * HD
    nq = qw // HD
    scale = HD ** (-0.5)
    me = lax.axis_index("context")
    rank = lax.rem(me, SEQ)
    base = me - rank
    my_seq = base // SEQ
    lead = lax.rem(rank, 2) == 0
    near = lax.rem(rank, 2) == 1

    def flip(bit):
        if bit == 1:
            return rank + 1 - 2 * lax.rem(rank, 2)
        if bit == 2:
            return lax.rem(rank + 2, 4)
        return 3 - rank

    peer = {j: base + flip(j) for j in (1, 2, 3)}
    zpeer = [lax.rem(my_seq + i, n_seq) * SEQ + rank for i in range(1, n_seq)]

    def rcopy(src, dst, ss, rs, dev):
        return pltpu.make_async_remote_copy(
            src_ref=src, dst_ref=dst, send_sem=ss, recv_sem=rs,
            device_id={"context": dev}, device_id_type=pl.DeviceIdType.MESH,
        )

    def tell(sem, dev):
        pl.semaphore_signal(sem, inc=1, device_id={"context": dev}, device_id_type=pl.DeviceIdType.MESH)

    barrier = pltpu.get_barrier_semaphore()

    @pl.when(lead)
    def _():
        tell(barrier, peer[1])
        tell(barrier, peer[3])
        for z in zpeer:
            tell(barrier, z)

    @pl.when(jnp.logical_not(lead))
    def _():
        tell(barrier, peer[2])

    pairs = [
        (k_h, k_in), (layout_h, layout), (t_start_h, t_start), (t_off_h, t_off), (kgain_h, kgain),
        (seg_h, seg), (qgain_h, qgain), (q_h, q_in), (g_h, g_in),
    ]
    loads = [pltpu.make_async_copy(a, b, l_sem.at[i]) for i, (a, b) in enumerate(pairs)]
    v_loads = [
        pltpu.make_async_copy(v_h.at[:, pl.ds(h * HD, HD)], kv.at[h, 0, 1], v_sem) for h in range(KVH)
    ]
    for c in loads[:5] + v_loads + loads[5:]:
        c.start()

    owners = [me, peer[2], peer[1], peer[3]]

    def factors(j):
        for i in range(spans):
            span = lax.rem(layout[owners[j] * spans + i], per_seq)
            c1, s1 = t_start[0, pl.ds(span, 1), :], t_start[1, pl.ds(span, 1), :]
            c2, s2 = t_off[0], t_off[1]
            cs[j, 0, i * SPAN : (i + 1) * SPAN, :] = c1 * c2 - s1 * s2
            cs[j, 1, i * SPAN : (i + 1) * SPAN, :] = s1 * c2 + c1 * s2

    def rot(x):
        return x * cs[0, 0] + pltpu.roll(x, HD // 2, 1) * cs[0, 1]

    def unrot(x, j=0):
        return x * cs[j, 0] - pltpu.roll(x, HD // 2, 1) * cs[j, 1]

    for c in loads[:5]:
        c.wait()
    factors(0)
    kf = k_in[...].astype(F32)
    rk = lax.rsqrt(jnp.sum(kf * kf, axis=1, keepdims=True) / kw + EPS)

    def x_copy(h, t):
        return rcopy(kv.at[h, 0, t], kv.at[h, 1, t], s_x, r_x.at[h], peer[2])

    def c_copy(h):
        return rcopy(kv.at[h, 0], kv.at[h, 2], s_c, r_cf.at[h], peer[1])

    def f_copy(h):
        return rcopy(kv.at[h, 1], kv.at[h, 3], s_f, r_cf.at[h], peer[1])

    def copy13(h):
        return rcopy(rs13.at[h], rr13.at[h], s_13, r_13.at[h], peer[1])

    def copy2(h):
        return rcopy(rs2.at[h], rr2.at[h], s_2, r_2.at[h], peer[2])

    def prepare_k(h):
        x = k_in[:, h * HD : (h + 1) * HD].astype(F32) * rk * kgain[h : h + 1, :]
        kv[h, 0, 0] = rot(x).astype(BF16)

    for h in range(AHEAD):
        prepare_k(h)
    pltpu.make_async_copy(kv.at[:, 0, 1], kv.at[:, 0, 1], v_sem).wait()

    @pl.when(jnp.logical_not(lead))
    def _():
        pl.semaphore_wait(barrier, 3)
        tell(ready, peer[1])

    @pl.when(lead)
    def _():
        pl.semaphore_wait(ready, 1)

    for h in range(KVH):
        if h >= AHEAD:
            prepare_k(h)
        x_copy(h, 1).start()
        x_copy(h, 0).start()
        c_copy(h).start()
    for c in loads[5:]:
        c.wait()
    for j in (1, 2, 3):
        factors(j)

    lane = lax.broadcasted_iota(jnp.int32, (1, HD), 1)
    sub = lax.broadcasted_iota(jnp.int32, (rows, 1), 0)

    def docs_of(owner):
        row = jnp.zeros((1, HD), jnp.int32)
        for i in range(spans):
            sp = layout[owner * spans + i]
            src = seg[pl.ds(sp // 2, 1), :]
            swp = pltpu.roll(src, SPAN, 1)
            want = jnp.where(lax.rem(sp, 2) == i, src, swp)
            row = jnp.where(lane // SPAN == i, want, row)
        return row

    def pos_of(owner, idx):
        out = idx
        for i in range(spans):
            out = jnp.where(idx // SPAN == i, layout[owner * spans + i] * SPAN + idx - i * SPAN, out)
        return out

    doc_q = docs_of(me)
    pos_q = pos_of(me, lane)
    doc_rows = jnp.concatenate(
        [docs_of(o).astype(F32) for o in owners] + [jnp.zeros((4, HD), F32)], axis=0
    )
    doc_cols = jnp.transpose(doc_rows)
    doc_qf = doc_q.astype(F32)
    for j in range(SEQ):
        ok = (doc_cols[:, j : j + 1] == doc_qf) & (pos_of(owners[j], sub) <= pos_q)
        bias[j * rows : (j + 1) * rows, :] = jnp.where(ok, 0.0, -jnp.inf).astype(F32)

    ssq = jnp.zeros((rows, HD), F32)
    for i in range(nq):
        x = q_in[:, i * HD : (i + 1) * HD].astype(F32)
        ssq = ssq + x * x
    rq = lax.rsqrt(jnp.sum(ssq, axis=1, keepdims=True) / qw + EPS)
    rqb[...] = jnp.broadcast_to(rq, (rows, HD))
    accq[...] = jnp.zeros((rows, HD), F32)

    def prepare_q(h, carry):
        for g in range(group):
            at = pl.multiple_of(h * gw + g * HD, HD)
            x = q_in[:, pl.ds(at, HD)].astype(F32) * rqb[...] * qgain[pl.ds(h * group + g, 1), :]
            qs[h, g * rows : (g + 1) * rows, :] = rot(x).astype(BF16)
            gs[h, g * rows : (g + 1) * rows, :] = g_in[:, pl.ds(at, HD)]
        return carry

    lax.fori_loop(0, KVH, prepare_q, 0)

    nt = (((1,), (1,)), ((), ()))
    tn = (((0,), (0,)), ((), ()))
    chunks = [(a, min(a + CHUNK, group)) for a in range(0, group, CHUNK)]

    def forward(h):
        rcopy(kv.at[h, 0], kv.at[h, 1], s_x, r_x.at[h], peer[2]).wait_recv()
        f_copy(h).start()

    def arrive(h):
        rcopy(kv.at[h, pl.ds(0, 2)], kv.at[h, pl.ds(2, 2)], s_c, r_cf.at[h], peer[1]).wait_recv()

    def relay(h):
        copy13(h).wait_recv()
        rs2[h] = (r2[h] + rr13[h, 1].astype(F32)).astype(BF16)
        r0[h] = r0[h] + rr13[h, 0].astype(F32)
        copy2(h).start()

    def scores(h, a, b):
        keys = kv[h, :, 0].reshape(SEQ * rows, HD)
        vals = kv[h, :, 1].reshape(SEQ * rows, HD)
        cols = slice(a * rows, b * rows)
        s = lax.dot_general(keys, qs[h, cols, :], nt, preferred_element_type=F32)
        dp = lax.dot_general(vals, gs[h, cols, :], nt, preferred_element_type=F32)
        return s, dp

    def weights(s, dp, a, b, ds_ref, p_ref):
        cols = slice(a * rows, b * rows)
        s = s * (scale * math.log2(math.e)) + jnp.concatenate([bias[...]] * (b - a), axis=1)
        e = jnp.exp2(s - jnp.max(s, axis=0, keepdims=True))
        inv = 1.0 / jnp.sum(e, axis=0, keepdims=True)
        delta = jnp.sum(e * dp, axis=0, keepdims=True) * inv
        p = e * inv
        ds_ref[:, cols] = (p * (dp - delta)).astype(BF16)
        p_ref[:, cols] = p.astype(BF16)

    def softmax(h, ds_ref, p_ref):
        for a, b in chunks:
            weights(*scores(h, a, b), a, b, ds_ref, p_ref)

    def key_products(h, ds_ref, p_ref):
        dk = jnp.dot(ds_ref[...], qs[h], preferred_element_type=F32) * scale
        r0[h, 0] = dk[:rows]
        r2[h, 0] = dk[rows : 2 * rows]
        rs13[h, 0, 0] = dk[2 * rows : 3 * rows].astype(BF16)
        rs13[h, 1, 0] = dk[3 * rows :].astype(BF16)
        return dk

    def key_gains(h, dk):
        kpart = jnp.zeros((rows, HD), F32)
        for j in range(SEQ):
            kpart = kpart + unrot(dk[j * rows : (j + 1) * rows], j) * unrot(kv[h, j, 0].astype(F32), j)
        gz[my_seq, h, group : group + 1, :] = jnp.sum(kpart, axis=0, keepdims=True) / kgain[pl.ds(h, 1), :]

    def value_products(h, p_ref):
        dv = jnp.dot(p_ref[...], gs[h], preferred_element_type=F32)
        r0[h, 1] = dv[:rows]
        r2[h, 1] = dv[rows : 2 * rows]
        rs13[h, 0, 1] = dv[2 * rows : 3 * rows].astype(BF16)
        rs13[h, 1, 1] = dv[3 * rows :].astype(BF16)

    def query_products(h, ds_ref):
        keys = kv[h, :, 0].reshape(SEQ * rows, HD)
        return lax.dot_general(keys, ds_ref[...], tn, preferred_element_type=F32) * scale

    def query_side(h, dq_t):
        acc = accq[...]
        for g in range(group):
            at = pl.multiple_of(h * gw + g * HD, HD)
            dqn = unrot(jnp.transpose(dq_t[:, g * HD : (g + 1) * HD]))
            x = q_in[:, pl.ds(at, HD)].astype(F32)
            w = dqn * qgain[pl.ds(h * group + g, 1), :]
            u[:, pl.ds(at, HD)] = w
            acc = acc + w * x
            gz[my_seq, h, g : g + 1, :] = jnp.sum(dqn * x * rqb[...], axis=0, keepdims=True)
        accq[...] = acc

    early_rows = pl.ds(0, KVH - 2)
    slot = my_seq * 2 + lax.rem(rank, 2)
    side = [peer[1]]
    for i in range(1, n_seq):
        side += [zpeer[i - 1], zpeer[i - 1] - rank + flip(1)]

    def z_copy(i):
        mine = gz.at[my_seq, early_rows]
        return rcopy(mine, mine, s_z.at[0], r_z.at[0], zpeer[i])

    def z_all():
        others = gz.at[pl.ds(0, n_seq - 1), early_rows]
        return rcopy(others, others, s_z.at[0], r_z.at[0], zpeer[0])

    def last_copy(dev):
        return rcopy(gz.at[my_seq, pl.ds(KVH - 2, 2)], glz.at[slot], s_z.at[1], r_z.at[1], dev)

    def last_all():
        others = glz.at[pl.ds(0, 2 * n_seq - 1)]
        return rcopy(others, others, s_z.at[1], r_z.at[1], peer[1])

    slots = ((ds_a, p_a), (ds_b, p_b))

    def step(h, now, nxt):
        sc = scores(h + 1, *chunks[0])
        dq_t = query_products(h, now[0])
        weights(*sc, *chunks[0], *nxt)
        sc = scores(h + 1, *chunks[1])
        dk = key_products(h, *now)
        query_side(h, dq_t)
        weights(*sc, *chunks[1], *nxt)
        value_products(h, now[1])
        key_gains(h, dk)
        copy13(h).start()

    def meet(h):
        forward(h + 1)
        arrive(h)

    forward(0)
    arrive(0)
    softmax(0, *slots[0])
    forward(1)

    def two(i, carry):
        h = 2 * i

        @pl.when(jnp.logical_and(lead, i == half - 1))
        def _():
            pl.semaphore_wait(z_ready, n_seq - 1)
            tell(z_known, peer[1])

        meet(h + 1)

        @pl.when(i > 0)
        def _():
            relay(h - 2)

        step(h, slots[0], slots[1])
        meet(h + 2)

        @pl.when(i > 0)
        def _():
            relay(h - 1)

        step(h + 1, slots[1], slots[0])
        return carry

    @pl.when(lead)
    def _():
        pl.semaphore_wait(barrier, n_seq - 1)
        for z in zpeer:
            tell(z_ready, z)

    half = (KVH - 2) // 2
    lax.fori_loop(0, half, two, 0)

    @pl.when(jnp.logical_not(lead))
    def _():
        pl.semaphore_wait(z_known, 1)

    for i in range(n_seq - 1):
        z_copy(i).start()
    arrive(KVH - 1)
    relay(KVH - 4)
    step(KVH - 2, slots[0], slots[1])

    dq_last = query_products(KVH - 1, slots[1][0])
    dk_last = key_products(KVH - 1, *slots[1])
    query_side(KVH - 1, dq_last)
    key_gains(KVH - 1, dk_last)
    glz[slot] = gz[my_seq, KVH - 2 :]
    for dev in side:
        last_copy(dev).start()
    relay(KVH - 3)
    relay(KVH - 2)
    value_products(KVH - 1, slots[1][1])
    copy13(KVH - 1).start()

    def gc_copy():
        return rcopy(gseq.at[0], gseq.at[1], s_g.at[0], r_g.at[0], peer[1])

    def gx_copy():
        return rcopy(gseq.at[2], gseq.at[3], s_g.at[1], r_g.at[1], peer[2])

    def gl_copy(j):
        return rcopy(glast.at[0], glast.at[1], s_l, r_l, peer[j])

    relay(KVH - 1)
    rq = rqb[...]
    inner = jnp.sum(accq[...], axis=1, keepdims=True) / qw * rq * rq * rq
    for i in range(nq):
        sl = slice(i * HD, (i + 1) * HD)
        qg_out[:, sl] = (rq * u[:, sl] - q_in[:, sl].astype(F32) * inner).astype(BF16)

    kacc = jnp.zeros((rows, HD), F32)

    def finish(h, kacc):
        sl = slice(h * HD, (h + 1) * HD)
        copy2(h).wait_recv()
        vg_out[:, sl] = (r0[h, 1] + rr2[h, 1].astype(F32)).astype(BF16)
        dkn = unrot(r0[h, 0] + rr2[h, 0].astype(F32))
        x = k_in[:, sl].astype(F32)
        w = dkn * kgain[h : h + 1, :]
        r2[h, 0] = w
        return kacc + w * x

    rcopy(kv.at[:, 0], kv.at[:, 1], s_x, r_x.at[0], peer[2]).wait_send()
    rcopy(kv.at[:, 0], kv.at[:, 2], s_c, r_cf.at[0], peer[1]).wait_send()
    rcopy(kv.at[:, 1], kv.at[:, 3], s_f, r_cf.at[0], peer[1]).wait_send()
    rcopy(rs13, rr13, s_13, r_13.at[0], peer[1]).wait_send()

    for h in range(3):
        kacc = finish(h, kacc)
    z_all().wait_recv()
    total = gz[0, early_rows]
    for s_i in range(1, n_seq):
        total = total + gz[s_i, early_rows]
    gseq[0] = total
    gc_copy().start()
    kacc = finish(3, kacc)
    kacc = finish(4, kacc)
    gc_copy().wait_recv()
    gseq[2] = gseq[0] + gseq[1]
    gx_copy().start()
    kacc = finish(KVH - 3, kacc)
    last_all().wait_recv()
    last = glz[0]
    for s_i in range(1, 2 * n_seq):
        last = last + glz[s_i]
    glast[0] = last

    @pl.when(near)
    def _():
        gl_copy(2).start()
        gl_copy(3).start()

    kacc = finish(KVH - 2, kacc)
    kacc = finish(KVH - 1, kacc)

    kinner = jnp.sum(kacc, axis=1, keepdims=True) / kw * rk * rk * rk
    for h in range(KVH):
        sl = slice(h * HD, (h + 1) * HD)
        kg_out[:, sl] = (rk * r2[h, 0] - k_in[:, sl].astype(F32) * kinner).astype(BF16)

    rcopy(rs2, rr2, s_2, r_2.at[0], peer[2]).wait_send()
    gc_copy().wait_send()
    z_all().wait_send()
    last_all().wait_send()

    def gains(h, rows_h):
        qgg_out[h * group : (h + 1) * group, :] = rows_h[:group]
        kgg_out[h : h + 1, :] = rows_h[group : group + 1]

    gx_copy().wait_recv()
    for h in range(KVH - 2):
        gains(h, gseq[2, h] + gseq[3, h])
    gx_copy().wait_send()
    gl_copy(2).wait_recv()
    for h in range(2):
        gains(KVH - 2 + h, glast[0, h] + glast[1, h])

    @pl.when(near)
    def _():
        rcopy(glast, glast, s_l, r_l, peer[2]).wait_send()


def flush(*refs):
    sems = refs[10]
    copies = [pltpu.make_async_copy(refs[i], refs[5 + i], sems.at[i]) for i in range(5)]
    for c in copies:
        c.start()
    for c in copies:
        c.wait()


def body(n_ctx, query_proj, key_proj, values, grad_out, query_gain, key_gain, segments, layout):
    rows, qw = query_proj.shape
    kw = key_proj.shape[1]
    group = qw // kw
    n_seq = n_ctx // SEQ
    nq, nk = qw // HD, kw // HD
    t_off, t_start = rope_tables()
    vmem = pl.BlockSpec(memory_space=pltpu.VMEM)
    sem = pltpu.SemaphoreType.DMA
    outs = pl.pallas_call(
        functools.partial(kernel, n_seq),
        out_shape=(
            pltpu.VMEM((rows, qw), BF16),
            pltpu.VMEM((rows, kw), BF16),
            pltpu.VMEM((rows, kw), BF16),
            pltpu.VMEM((nq, HD), F32),
            pltpu.VMEM((nk, HD), F32),
        ),
        in_specs=[pl.BlockSpec(memory_space=pltpu.HBM)] * 10,
        out_specs=(vmem,) * 5,
        scratch_shapes=[
            pltpu.VMEM((nk, SEQ, 2, rows, HD), BF16),
            pltpu.VMEM((SEQ * rows, rows), F32),
            pltpu.VMEM((SEQ, 2, rows, HD), F32),
            pltpu.VMEM((nk, group * rows, HD), BF16),
            pltpu.VMEM((nk, group * rows, HD), BF16),
            pltpu.VMEM((rows, qw), F32),
            pltpu.VMEM((nk, 2, rows, HD), F32),
            pltpu.VMEM((nk, 2, rows, HD), F32),
            pltpu.VMEM((nk, 2, 2, rows, HD), BF16),
            pltpu.VMEM((nk, 2, 2, rows, HD), BF16),
            pltpu.VMEM((nk, 2, rows, HD), BF16),
            pltpu.VMEM((nk, 2, rows, HD), BF16),
            pltpu.VMEM((SEQ, nk - 2, group + 1, HD), F32),
            pltpu.VMEM((n_seq, nk, group + 1, HD), F32),
        ]
        + [pltpu.VMEM((SEQ * rows, group * rows), BF16)] * 4
        + [pltpu.VMEM((rows, HD), F32)] * 2
        + [pltpu.VMEM((2, 2, group + 1, HD), F32), pltpu.VMEM((2 * n_seq, 2, group + 1, HD), F32)]
        + [sem] * 7
        + [sem((nk,))] * 4
        + [sem((2,))] * 4
        + [
            pltpu.SMEM(layout.shape, jnp.int32),
            pltpu.VMEM((segments.shape[0] // HD, HD), jnp.int32),
            pltpu.VMEM((rows, qw), BF16),
            pltpu.VMEM((rows, kw), BF16),
            pltpu.VMEM((rows, qw), BF16),
            pltpu.VMEM((nq, HD), F32),
            pltpu.VMEM((nk, HD), F32),
            pltpu.VMEM(t_off.shape, F32),
            pltpu.VMEM(t_start.shape, F32),
            sem((9,)),
            sem,
        ]
        + [pltpu.SemaphoreType.REGULAR] * 3,
        compiler_params=pltpu.CompilerParams(
            collective_id=0, has_side_effects=True, vmem_limit_bytes=65100000
        ),
    )(
        layout, segments.reshape(-1, HD), query_proj, key_proj, values, grad_out,
        query_gain.reshape(nq, HD), key_gain.reshape(nk, HD), jnp.asarray(t_off), jnp.asarray(t_start),
    )
    anyspace = pl.BlockSpec(memory_space=pl.ANY)
    outs = pl.pallas_call(
        flush,
        out_shape=tuple(jax.ShapeDtypeStruct(o.shape, o.dtype) for o in outs),
        in_specs=[anyspace] * 5,
        out_specs=(anyspace,) * 5,
        scratch_shapes=[sem((5,))],
        compiler_params=pltpu.CompilerParams(vmem_limit_bytes=8 * 1024 * 1024),
    )(*outs)
    return outs[0], outs[1], outs[2], outs[3].reshape(qw), outs[4].reshape(kw)


def solution(mesh):
    tok = P(("groups", "context"), None)
    return jax.shard_map(
        functools.partial(body, mesh.shape["context"]),
        mesh=mesh,
        in_specs=(tok, tok, tok, tok, P(), P(), P("groups"), P("groups")),
        out_specs=(tok, tok, tok, P("groups"), P("groups")),
        check_vma=False,
    )
```
